128 devices in a mesh: expert: 8 (over y, x_lo), ffn: 16 (over z, x_hi, core).
Axes of the slice: x: 4 (x_hi: 2, x_lo: 2; x = x_hi * 2 + x_lo), y: 4, z: 4, core: 2. Of those that a mesh axis runs over, the one named last changes fastest.
Arguments:
- tokens: bfloat16 [2048, 4096], P('expert'), may hold values from -6 to 6
- router_gates: float32 [2048, 2], P('expert'), may hold values from 0.1 to 1
- routes: int32 [2048, 2], P('expert'), may hold values from 0 to 7, all different within a row; in each aligned block of 256 rows (0 to 255, 256 to 511, ...) at most 128 rows name the same one
- gate_proj: bfloat16 [8, 4096, 14336], P('expert', None, 'ffn'), may hold values from -0.09375 to 0.09375
- up_proj: bfloat16 [8, 4096, 14336], P('expert', None, 'ffn'), may hold values from -0.09375 to 0.09375
- down_proj: bfloat16 [8, 14336, 4096], P('expert', 'ffn'), may hold values from -0.0625 to 0.0625
Outputs:
- mixed: bfloat16 [2048, 4096], P('expert', 'ffn')
The draws below stay inside these ranges and needn't reach their ends.
Inputs may be any that keep to these rules, and one draw needn't show every extreme that they name: `routes`: the 2 experts of a token differ. Among the tokens of one index of the expert axis (aligned blocks of 256 tokens) no expert is chosen by more than 128 tokens, and in some blocks one expert is chosen by exactly 128.
All inputs are finite; a program needn't handle non-finite values.
Results may differ from the reference program's by a relative error of at most 0.017.
Values may be sent and summed in bfloat16 or wider, within the bound.
A program may use at most 128 MiB of HBM per device.

```python
import math
import jax
import jax.numpy as jnp
import numpy as np
from jax import lax

D = 4096
FF = 14336
TOP = 2
TOK_DEV = 256
EXPERTS = 8
CAP = 128
TOKENS = 2048
N_FFN = 16


def strengthened(values, rng, source, target, parts, factor):
    def block_of(dim):
        return (jnp.arange(values.shape[dim]) // (values.shape[dim] // parts)).reshape((-1,) + (1,) * (values.ndim - 1 - dim))

    one_side = jax.random.permutation(rng, parts)[block_of(target)]
    other_side = (block_of(target) + parts // 2) % parts
    return jnp.where((block_of(source) == one_side) | (block_of(source) == other_side), factor * values, values)


def steps_of(key, dims, pieces, low, high):
    loudness = 1.0
    for axis_at, shards_of in pieces:
        steps = jax.random.uniform(jax.random.fold_in(jax.random.fold_in(key, 6), axis_at), (shards_of,), jnp.float32, low / len(pieces), high / len(pieces))
        loudness = loudness * jnp.repeat(jnp.exp(steps), dims[axis_at] // shards_of).reshape((-1,) + (1,) * (len(dims) - 1 - axis_at))
    return loudness


def shared_out(key, own, number, rows, count, top, limit, lean):
    sequence = jax.random.permutation(key, count)
    crowded, ordinary = load_shares(count, rows * top, limit, lean, True), load_shares(count, rows * top, limit, lean, False)
    places = jnp.arange(count)

    def named(lengths, offset_by):
        used = int((lengths > 0).sum())
        fixed = max(1, used // 4)
        passed = fixed + (places - fixed + offset_by * (used - fixed)) % max(1, count - fixed)
        return jnp.zeros((count,), jnp.int32).at[sequence[jnp.where(places < fixed, places, passed)]].set(jnp.asarray(lengths, jnp.int32))

    lengths = jnp.where(number % 4 == 0, named(crowded, number // 4), named(ordinary, number - number // 4 - 1))
    mixed = jax.random.permutation(jax.random.fold_in(own, 3), count)
    source_of, taker = mixed[0:count // 2 * 2:2], mixed[1:count // 2 * 2:2]
    slack = jnp.minimum(lengths[source_of] - 1, limit - lengths[taker]) // 2
    slack = jnp.where((source_of == sequence[0]) | (taker == sequence[0]) | (lengths[taker] == 0), 0, jnp.maximum(slack, 0))
    passed = jax.random.randint(jax.random.fold_in(own, 4), (count // 2,), 0, 1 << 20) % (slack + 1)
    lengths = lengths.at[source_of].add(-passed).at[taker].add(passed)
    labels = jnp.searchsorted(jnp.cumsum(lengths), jnp.arange(rows * top), side="right").astype(jnp.int32)
    grid = labels.reshape(top, rows).T
    grid = grid[jax.random.permutation(jax.random.fold_in(own, 1), rows)]
    offset_by = jax.random.randint(jax.random.fold_in(own, 2), (rows, 1), 0, top)
    return jnp.take_along_axis(grid, (jnp.arange(top)[None, :] + offset_by) % top, axis=1)


def load_shares(number_of, total, reach, lean, full):
    weights = [(1 << 20) // math.isqrt(standing ** lean) + 1 for standing in range(1, number_of + 1)]
    largest = reach if full else min(reach, max(-(-total // number_of), total * weights[0] // sum(weights)))
    least = 1 if total - largest >= number_of - 1 else 0
    holding, surplus = [largest] + [least] * (number_of - 1), total - largest - least * (number_of - 1)
    while surplus > 0:
        free = [i for i in range(1, number_of) if holding[i] < largest] or [i for i in range(1, number_of) if holding[i] < reach]
        pool, budget = sum([weights[i] for i in free]), surplus
        for i in free:
            extra = min(reach - holding[i], max(1, budget * weights[i] // pool), surplus)
            holding[i] = holding[i] + extra
            surplus = surplus - extra
    return np.array(holding)


def centred(own_key, shape, deviation, most, shards=(), kind=jnp.bfloat16):
    entries = deviation * jax.random.normal(own_key, shape, jnp.float32)
    if shards:
        entries = entries * steps_of(own_key, shape, shards, -0.22, 0.18)
    return jnp.clip(entries, -most, most).astype(kind)


def gaussian_with(own_key, extent, spread, bound, cuts, heavy, kind=jnp.bfloat16):
    drawn = spread * jax.random.normal(own_key, extent, jnp.float32)
    if cuts:
        drawn = drawn * steps_of(own_key, extent, cuts, -0.22, 0.18)
    return jnp.clip(strengthened(drawn, jax.random.fold_in(own_key, 3), *heavy), -bound, bound).astype(kind)


def setup_inputs(seed: int = 0) -> dict:
    streams_of = jax.random.split(jax.random.key(seed), 7)
    tokens = centred(streams_of[0], (TOKENS, D), 1.0, 6.0, ((0, 8),))
    router_gates = jnp.clip(jnp.exp(math.log(1.0) - 2.3025851 * jax.random.uniform(streams_of[1], (TOKENS, TOP), jnp.float32) ** steps_of(streams_of[1], (TOKENS, TOP), ((0, 8),), -0.2, 0.2)), 0.1, 1.0)
    routes_keys = jax.random.split(jax.random.fold_in(streams_of[2], 1), TOKENS // TOK_DEV)
    routes_turns = jax.random.permutation(jax.random.fold_in(streams_of[2], 3), TOKENS // TOK_DEV)
    routes = jax.vmap(lambda own, number: shared_out(jax.random.fold_in(streams_of[2], 2), own, number, TOK_DEV, EXPERTS, TOP, CAP, 2))(routes_keys, routes_turns).reshape((TOKENS, TOP))
    gate_proj = centred(streams_of[3], (EXPERTS, D, FF), D ** -0.5, 0.09375, ((0, 8), (2, 16)))
    up_proj = centred(streams_of[4], (EXPERTS, D, FF), D ** -0.5, 0.09375, ((0, 8), (2, 16)))
    down_proj = gaussian_with(streams_of[5], (EXPERTS, FF, D), FF ** -0.5, 0.0625, ((0, 8), (1, 16)), (1, 2, 16, 2.0))
    return {"tokens": tokens, "router_gates": router_gates, "routes": routes, "gate_proj": gate_proj, "up_proj": up_proj, "down_proj": down_proj}


def slot_numbers(routes):
    grouped = routes.reshape(-1, TOK_DEV * TOP)
    chosen = (grouped[:, :, None] == jnp.arange(EXPERTS, dtype=jnp.int32)[None, None, :]).astype(jnp.int32)
    ranking = jnp.cumsum(chosen, axis=1) - chosen
    return jnp.sum(ranking * chosen, axis=2).reshape(-1, TOP).astype(jnp.int32)


def run_expert(operands):
    buffer_rows, gate_matrix, up_matrix, down_matrix = operands
    gate_act = jnp.dot(buffer_rows, gate_matrix, preferred_element_type=jnp.float32)
    up_act = jnp.dot(buffer_rows, up_matrix, preferred_element_type=jnp.float32)
    hidden = (jax.nn.silu(gate_act) * up_act).astype(jnp.bfloat16)
    shard_width = FF // N_FFN

    def add_shard(running, shard_index):
        hidden_part = lax.dynamic_slice_in_dim(hidden, shard_index * shard_width, shard_width, 1)
        down_part = lax.dynamic_slice_in_dim(down_matrix, shard_index * shard_width, shard_width, 0)
        rounded = jnp.dot(hidden_part, down_part, preferred_element_type=jnp.float32).astype(jnp.bfloat16)
        rounded = lax.optimization_barrier(rounded)
        return running + rounded.astype(jnp.float32), None

    start_sum = jnp.zeros((buffer_rows.shape[0], D), jnp.float32)
    result, unused = lax.scan(add_shard, start_sum, jnp.arange(N_FFN, dtype=jnp.int32))
    return result


def reference(tokens, router_gates, routes, gate_proj, up_proj, down_proj):
    sources = TOKENS // TOK_DEV
    slot = slot_numbers(routes)
    owner = (jnp.arange(TOKENS, dtype=jnp.int32) // TOK_DEV)[:, None]
    position = (owner * CAP + slot).astype(jnp.int32)
    buffers = jnp.zeros((EXPERTS, sources * CAP, D), jnp.bfloat16)
    buffers = buffers.at[routes, position].set(jnp.broadcast_to(tokens[:, None, :], (TOKENS, TOP, D)))
    outputs = lax.map(run_expert, (buffers, gate_proj, up_proj, down_proj))
    picked = outputs[routes, position]
    mixed = jnp.sum(router_gates[:, :, None] * picked, axis=1)
    return mixed.astype(jnp.bfloat16)
```

```python
import jax
import jax.numpy as jnp
from jax import lax
from jax.experimental import pallas as pl
from jax.experimental.pallas import tpu as pltpu
from jax.sharding import PartitionSpec as P

TOP = 2
MESH = pl.DeviceIdType.MESH
REL = ((0, 0), (0, 1), (1, 0), (3, 0), (1, 1), (3, 1), (2, 0), (2, 1))
CHUNKS = ((0, 1), (2, 3), (6, 7), (4, 5))
F32 = jnp.float32
BF16 = jnp.bfloat16


def dot(a, b):
    return jnp.dot(a, b, preferred_element_type=F32)


def kernel(
    tok_hbm, placing, weighting, gate_hbm, up_hbm, down_hbm, out_ref,
    X, Wg, Wu, Wd, tok, OB, OP, hid, part, rD, rA1, rA2, rAx, rBx, rB1, rB2, G,
    send_sem, recv_sem, local_sem,
):
    e = lax.axis_index("expert")
    f = lax.axis_index("ffn")
    y, xl = e // 2, e % 2
    z, xh, c = f // 4, (f // 2) % 2, f % 2
    x = xh * 2 + xl

    def at(yy, xx, zz, cc):
        yy, xx, zz = yy % 4, xx % 4, zz % 4
        return {"expert": yy * 2 + xx % 2, "ffn": zz * 4 + (xx // 2) * 2 + cc}

    loads = [
        pltpu.make_async_copy(s, d, local_sem.at[i])
        for i, (s, d) in enumerate(((tok_hbm, tok), (gate_hbm, Wg), (up_hbm, Wu), (down_hbm, Wd)))
    ]
    for cp in loads:
        cp.start()

    barrier = pltpu.get_barrier_semaphore()
    peers = [
        at(y, x, z, 1 - c), at(y, x + 1, z, c), at(y, x + 3, z, c), at(y, x + 2, z, c),
        at(y + 1, x, z, c), at(y + 3, x, z, c), at(y + 2, x, z, c),
        at(y + 1, x + 1, z, c), at(y + 1, x + 3, z, c), at(y + 3, x + 1, z, c), at(y + 3, x + 3, z, c),
        at(y + 2, x + 1, z, c), at(y + 2, x + 3, z, c), at(y, x, z + 1, c), at(y, x, z + 3, c),
    ]
    for dev in peers:
        pl.semaphore_signal(barrier, inc=1, device_id=dev, device_id_type=MESH)
    pl.semaphore_wait(barrier, len(peers))

    copies = []

    def send(src, dst, dev):
        i = len(copies)
        cp = pltpu.make_async_remote_copy(
            src_ref=src, dst_ref=dst, send_sem=send_sem.at[i], recv_sem=recv_sem.at[i],
            device_id=dev, device_id_type=MESH,
        )
        cp.start()
        copies.append(cp)
        return cp

    other = at(y, x, z, 1 - c)
    half = pl.multiple_of(c * 2048, 2048)

    loads[0].wait()

    def place(t, carry):
        o = pl.multiple_of(t * 512, 512)
        v = dot(placing[128:768, :], tok[:, pl.ds(pl.multiple_of(half + o, 512), 512)])
        OB[:, pl.ds(o, 512)] = v.astype(BF16)
        return carry

    lax.fori_loop(0, 4, place, 0)
    x7 = (x + 1 + 2 * c) % 4
    block = c * 8 + z * 2 + xh
    block7 = c * 8 + z * 2 + x7 // 2

    def cols(b, width=256):
        return pl.ds(pl.multiple_of(b * 256, 256), width)

    OP[0] = dot(placing[768:896, :], tok[:, cols(block)]).astype(BF16)
    OP[1] = dot(placing[896:1024, :], tok[:, cols(block7)]).astype(BF16)

    def quarters(r, yy):
        got = []
        for i, step in enumerate((1, 3)):
            got.append(send(
                OB.at[(r - 1) * 128:r * 128, i * 1024:(i + 1) * 1024],
                X.at[r * 128:(r + 1) * 128, pl.ds(pl.multiple_of(half + i * 1024, 1024), 1024)],
                at(yy, x + step, z, c),
            ))
        return got

    def halves(r, yy):
        return [send(
            OB.at[(r - 1) * 128:r * 128, :],
            X.at[r * 128:(r + 1) * 128, pl.ds(half, 2048)],
            at(yy, x, z, c),
        )]

    arrive = {}
    arrive[1] = quarters(1, y)
    arrive[6] = [send(OP.at[0], X.at[768:896, cols(block)], at(y + 2, x, z, c))]
    arrive[7] = [send(OP.at[1], X.at[896:1024, cols(block7)], at(y + 2, x7, z, c))]
    arrive[2] = halves(2, y + 3)
    arrive[3] = halves(3, y + 1)
    arrive[4] = quarters(4, y + 3)
    arrive[5] = quarters(5, y + 1)

    def place_own(t, carry):
        o = pl.ds(pl.multiple_of(t * 512, 512), 512)
        X[0:128, o] = dot(placing[0:128, :], tok[:, o]).astype(BF16)
        return carry

    lax.fori_loop(0, 8, place_own, 0)

    def landed(cps):
        for cp in cps:
            cp.wait_recv()

    def forward(r):
        landed(arrive[r])
        where = X.at[r * 128:(r + 1) * 128, pl.ds(half, 2048)]
        return send(where, where, other)

    def spread(b, width, dev):
        where = X.at[768:1024, cols(b, width)]
        return send(where, where, dev)

    pair = lambda zz: c * 8 + (zz % 4) * 2
    xdev, up_z, dn_z = at(y, x + 2, z, c), at(y, x, z + 1, c), at(y, x, z + 3, c)

    landed(arrive[6] + arrive[7])
    ag1 = spread(block, 256, xdev)
    fwd1 = forward(1)
    ag1.wait_recv()
    ag2 = [spread(pair(z), 512, up_z), spread(pair(z), 512, dn_z)]
    core_pairs = [spread(pair(z), 512, other)]

    def gather_far():
        landed(ag2)
        far = [spread(pair(z + 3), 256, up_z), spread(pair(z + 1) + 1, 256, dn_z)]
        core_pairs.append(spread(pair(z + 1), 512, other))
        core_pairs.append(spread(pair(z + 3), 512, other))
        return far

    def gather_end(far):
        landed(far)
        core_pairs.append(spread(pair(z + 2), 512, other))

    def gate_up(k, lo, hi):
        row = CHUNKS[k][0] * 128
        rows = slice(row, row + 256)

        def tile(t, carry):
            o = cols(t)
            g = dot(X[rows, :], Wg[:, o])
            u = dot(X[rows, :], Wu[:, o])
            hid[:, o] = (g / (1.0 + jnp.exp(-g)) * u).astype(BF16)
            return carry

        lax.fori_loop(lo, min(hi, 3), tile, 0)
        if hi > 3:
            w = jnp.concatenate([Wg[:, 768:896], Wu[:, 768:896]], axis=1)
            gu = dot(X[rows, :], w)
            g, u = gu[:, :128], gu[:, 128:]
            hid[:, 768:896] = (g / (1.0 + jnp.exp(-g)) * u).astype(BF16)

    def down(k, cc):
        def tile(t, carry):
            for zi in range(2):
                for xi in range(2):
                    zz = t * 2 + zi
                    v = dot(hid[...], Wd[:, cols(zz * 4 + xi * 2 + cc)])
                    part[k, cc, zz, xi] = v.astype(BF16)
            return carry

        lax.fori_loop(0, 2, tile, 0)

    def add(dst, *srcs):
        total = dst[...].astype(F32)
        for s in srcs:
            total = total + s[...].astype(F32)
        dst[...] = total.astype(BF16)

    zp, zm, zf = (z + 1) % 4, (z + 3) % 4, (z + 2) % 4
    st = [dict() for _ in CHUNKS]

    def send_core(k):
        st[k]["d"] = send(part.at[k, 1 - c], rD.at[k], other)

    def s0(k):
        st[k]["d"].wait_recv()

        def body(zz, carry):
            for xi in range(2):
                add(part.at[k, c, zz, xi], rD.at[k, zz, xi])
            return carry

        lax.fori_loop(0, 4, body, 0)
        mine = part.at[k, c]
        st[k]["bx"] = send(mine.at[:, 1 - xh, 128:256], rBx.at[k], xdev)
        st[k]["a1"] = [
            send(mine.at[zf, 0, 0:128], rA1.at[k, 0], up_z),
            send(mine.at[zf, 1, 0:128], rA1.at[k, 1], dn_z),
        ]

    def s1(k):
        mine = part.at[k, c]
        landed(st[k]["a1"])
        add(mine.at[zp, 0, 0:128], rA1.at[k, 0])
        add(mine.at[zm, 1, 0:128], rA1.at[k, 1])
        st[k]["a2"] = [
            send(mine.at[zp, :, 0:128], rA2.at[k, 0], up_z),
            send(mine.at[zm, :, 0:128], rA2.at[k, 1], dn_z),
        ]
        st[k]["bx"].wait_recv()

        def body(zz, carry):
            add(mine.at[zz, xh, 128:256], rBx.at[k, zz])
            return carry

        lax.fori_loop(0, 4, body, 0)
        st[k]["b1"] = [
            send(mine.at[zf, xh, 128:192], rB1.at[k, 0], up_z),
            send(mine.at[zf, xh, 192:256], rB1.at[k, 1], dn_z),
        ]

    def s2(k):
        mine = part.at[k, c]
        landed(st[k]["a2"])
        add(mine.at[z, 1 - xh, 0:128], rA2.at[k, 0, 1 - xh], rA2.at[k, 1, 1 - xh])
        st[k]["ax"] = send(mine.at[z, 1 - xh, 0:128], rAx.at[k], xdev)
        landed(st[k]["b1"])
        add(mine.at[zp, xh, 128:192], rB1.at[k, 0])
        add(mine.at[zm, xh, 192:256], rB1.at[k, 1])
        st[k]["b2"] = [
            send(mine.at[zp, xh, 128:256], rB2.at[k, 0], up_z),
            send(mine.at[zm, xh, 128:256], rB2.at[k, 1], dn_z),
        ]

    returned = []

    def give_back(r, src):
        dy, dx = REL[r]
        if dy == 0 and dx == 0:
            G[r] = src[...]
            return
        owner = {"expert": ((y + dy) % 4) * 2 + (xl + dx) % 2, "ffn": f}
        returned.append(send(src, G.at[r], owner))

    def s3(k):
        mine = part.at[k, c]
        st[k]["ax"].wait_recv()
        add(mine.at[z, xh, 0:128], rA2.at[k, 0, xh], rA2.at[k, 1, xh], rAx.at[k])
        give_back(CHUNKS[k][0], mine.at[z, xh, 0:128])
        landed(st[k]["b2"])
        add(mine.at[z, xh, 128:256], rB2.at[k, 0], rB2.at[k, 1])
        give_back(CHUNKS[k][1], mine.at[z, xh, 128:256])

    loads[1].wait()
    loads[2].wait()
    fwd1.wait_recv()
    gate_up(0, 0, 4)
    loads[3].wait()
    down(0, 1 - c)
    send_core(0)
    down(0, c)
    fwd2 = [forward(2), forward(3)]
    far = gather_far()
    s0(0)
    landed(fwd2)
    gate_up(1, 0, 4)
    gather_end(far)
    s1(0)
    down(1, 1 - c)
    send_core(1)
    down(1, c)
    s2(0)
    s0(1)
    landed(core_pairs)
    gate_up(2, 0, 4)
    fwd3 = [forward(4), forward(5)]
    s3(0)
    s1(1)
    down(2, 1 - c)
    send_core(2)
    down(2, c)
    s2(1)
    s0(2)
    landed(fwd3)
    gate_up(3, 0, 2)
    s3(1)
    s1(2)
    gate_up(3, 2, 4)
    down(3, 1 - c)
    send_core(3)
    s2(2)
    down(3, c)
    s0(3)
    s3(2)
    s1(3)
    s2(3)
    s3(3)
    landed(returned)
    total = jnp.zeros(out_ref.shape, F32)
    for r in range(8):
        w = weighting[:, r * 128:(r + 1) * 128]
        hi = w.astype(BF16)
        lo = (w - hi.astype(F32)).astype(BF16)
        total = total + dot(hi, G[r]) + dot(lo, G[r])
    out_ref[...] = total.astype(BF16)
    for cp in copies:
        cp.wait_send()


N_COPIES = 80


def per_device(tokens, router_gates, routes, gate_proj, up_proj, down_proj):
    experts = lax.axis_size("expert")
    tok_rows, width = tokens.shape
    capacity = 2 * TOP * tok_rows // experts
    hidden = gate_proj.shape[2]
    e = lax.axis_index("expert")
    y, xl = e // 2, e % 2
    flattened = routes.reshape(-1)
    chosen = (flattened[:, None] == jnp.arange(experts, dtype=jnp.int32)[None, :]).astype(jnp.int32)
    ranking = jnp.cumsum(chosen, axis=0) - chosen
    targets = (flattened * capacity + jnp.sum(ranking * chosen, axis=1)).reshape(tok_rows, TOP)
    owners = jnp.stack([((y - dy) % 4) * 2 + (xl + dx) % 2 for dy, dx in REL]).astype(jnp.int32)
    slot_ids = (owners[:, None] * capacity + jnp.arange(capacity, dtype=jnp.int32)[None, :]).reshape(-1)
    first, second = targets[:, 0], targets[:, 1]
    placing = ((slot_ids[:, None] == first[None, :]) | (slot_ids[:, None] == second[None, :])).astype(BF16)
    weighting = jnp.where(first[:, None] == slot_ids[None, :], router_gates[:, 0:1], 0.0) + jnp.where(
        second[:, None] == slot_ids[None, :], router_gates[:, 1:2], 0.0
    )
    vmem = lambda *shape: pltpu.VMEM(shape, BF16)
    any_spec = pl.BlockSpec(memory_space=pl.ANY)
    vmem_spec = pl.BlockSpec(memory_space=pltpu.VMEM)
    return pl.pallas_call(
        kernel,
        out_shape=jax.ShapeDtypeStruct((tok_rows, 256), BF16),
        in_specs=[any_spec, vmem_spec, vmem_spec, any_spec, any_spec, any_spec],
        out_specs=vmem_spec,
        scratch_shapes=[
            vmem(1024, width), vmem(width, hidden), vmem(width, hidden), vmem(hidden, width),
            vmem(tok_rows, width), vmem(640, 2048), vmem(2, 128, 256), vmem(256, hidden),
            vmem(4, 2, 4, 2, 256, 256), vmem(4, 4, 2, 256, 256),
            vmem(4, 2, 128, 256), vmem(4, 2, 2, 128, 256), vmem(4, 128, 256),
            vmem(4, 4, 128, 256), vmem(4, 2, 64, 256), vmem(4, 2, 128, 256), vmem(8, 128, 256),
            pltpu.SemaphoreType.DMA((N_COPIES,)), pltpu.SemaphoreType.DMA((N_COPIES,)),
            pltpu.SemaphoreType.DMA((4,)),
        ],
        compiler_params=pltpu.CompilerParams(
            collective_id=0, has_side_effects=True, vmem_limit_bytes=67043328
        ),
        name="layer",
    )(tokens, placing, weighting, gate_proj[0], up_proj[0], down_proj[0])


def solution(mesh):
    in_specs = (
        P("expert", None),
        P("expert", None),
        P("expert", None),
        P("expert", None, "ffn"),
        P("expert", None, "ffn"),
        P("expert", "ffn", None),
    )
    out_specs = P("expert", "ffn")
    return jax.shard_map(
        per_device, mesh=mesh, in_specs=in_specs, out_specs=out_specs, check_vma=False
    )
```

```python
import jax
import jax.numpy as jnp
from jax import lax
from jax.experimental import pallas as pl
from jax.experimental.pallas import tpu as pltpu
from jax.sharding import PartitionSpec as P

MESH = pl.DeviceIdType.MESH
REL = ((0, 0), (0, 1), (1, 0), (3, 0), (2, 0), (2, 1), (1, 1), (3, 1))
CHUNKS = (
    (0, 128, 64, False), (128, 128, 64, False), (256, 256, 192, False), (512, 256, 128, False), (768, 128, 64, True), (896, 128, 64, True),
)
F32 = jnp.float32
BF16 = jnp.bfloat16


def dot(a, b):
    return jnp.dot(a, b, preferred_element_type=F32)


def kernel(
    tok_hbm, routes, gates, gate_hbm, up_hbm, down_hbm, out_ref,
    X, Wg, Wu, Wd, tok, OB, OP, hid, part, rD, rA1, rA2, rAx, rBx, rB1, rB2, rA3, rB3, G,
    placing, whi, wlo, keys, keyr, gater, mixed,
    send_sem, recv_sem, local_sem,
):
    e = lax.axis_index("expert")
    f = lax.axis_index("ffn")
    y, xl = e // 2, e % 2
    z, xh, c = f // 4, (f // 2) % 2, f % 2
    x = xh * 2 + xl

    def at(yy, xx, zz, cc):
        yy, xx, zz = yy % 4, xx % 4, zz % 4
        return {"expert": yy * 2 + xx % 2, "ffn": zz * 4 + (xx // 2) * 2 + cc}

    loads = [
        pltpu.make_async_copy(s, d, local_sem.at[i])
        for i, (s, d) in enumerate(((tok_hbm, tok), (gate_hbm, Wg), (up_hbm, Wu), (down_hbm, Wd)))
    ]
    for cp in loads:
        cp.start()

    barrier = pltpu.get_barrier_semaphore()
    peers = [
        at(y, x, z, 1 - c), at(y, x + 1, z, c), at(y, x + 3, z, c), at(y, x + 2, z, c),
        at(y + 1, x, z, c), at(y + 3, x, z, c), at(y + 2, x, z, c),
        at(y + 1, x + 1, z, c), at(y + 1, x + 3, z, c), at(y + 3, x + 1, z, c), at(y + 3, x + 3, z, c),
        at(y + 2, x + 1, z, c), at(y + 2, x + 3, z, c), at(y, x, z + 1, c), at(y, x, z + 3, c),
        at(y, x, z + 2, c),
    ]
    for dev in peers:
        pl.semaphore_signal(barrier, inc=1, device_id=dev, device_id_type=MESH)

    expert_ids = lax.broadcasted_iota(jnp.int32, (8, 256), 0)
    first, second = routes[0:1, :] == expert_ids, routes[1:2, :] == expert_ids
    chosen = jnp.where(first | second, 1.0, 0.0)
    earlier = lax.broadcasted_iota(jnp.int32, (256, 256), 0) < lax.broadcasted_iota(jnp.int32, (256, 256), 1)
    rank = dot(chosen.astype(BF16), jnp.where(earlier, 1.0, 0.0).astype(BF16))
    keys[0] = jnp.where(first | second, rank, -1.0)
    keys[1] = jnp.where(first, gates[0:1, :], 0.0) + jnp.where(second, gates[1:2, :], 0.0)
    row_ids = lax.broadcasted_iota(jnp.int32, (128, 256), 0).astype(F32)
    for r, (dy, dx) in enumerate(REL):
        owner = ((y + 4 - dy) % 4) * 2 + (xl + dx) % 2
        key = keys[0, pl.ds(owner, 1), :]
        keyr[r:r + 1, :] = key
        gater[r:r + 1, :] = keys[1, pl.ds(owner, 1), :]
        placing[r * 128:(r + 1) * 128, :] = jnp.where(key == row_ids, 1.0, 0.0).astype(BF16)

    copies = []

    def send(src, dst, dev):
        i = len(copies)
        cp = pltpu.make_async_remote_copy(
            src_ref=src, dst_ref=dst, send_sem=send_sem.at[i], recv_sem=recv_sem.at[i],
            device_id=dev, device_id_type=MESH,
        )
        cp.start()
        copies.append(cp)
        return cp

    other = at(y, x, z, 1 - c)
    half = pl.multiple_of(c * 2048, 2048)

    def cols(b, width=256):
        return pl.ds(pl.multiple_of(b * 256, 256), width)

    x5 = (x + 1 + 2 * c) % 4
    block = c * 8 + z * 2 + xh
    block5 = c * 8 + z * 2 + x5 // 2
    loads[0].wait()
    OP[0] = dot(placing[512:640, :], tok[:, cols(block)]).astype(BF16)
    OP[1] = dot(placing[640:768, :], tok[:, cols(block5)]).astype(BF16)

    def place(lo, hi):
        def tile(t, carry):
            o = pl.multiple_of(t * 1024, 1024)
            v = dot(placing[lo:hi, :], tok[:, pl.ds(pl.multiple_of(half + o, 1024), 1024)])
            OB[lo:hi, pl.ds(o, 1024)] = v.astype(BF16)
            return carry

        lax.fori_loop(0, 2, tile, 0)

    def place_own(t, carry):
        o = pl.ds(pl.multiple_of(t * 1024, 1024), 1024)
        X[0:128, o] = dot(placing[0:128, :], tok[:, o]).astype(BF16)
        return carry

    place(128, 512)
    place(768, 1024)
    lax.fori_loop(0, 4, place_own, 0)

    pl.semaphore_wait(barrier, len(peers))

    def quarter(r, yy, i):
        return send(
            OB.at[r * 128:(r + 1) * 128, i * 1024:(i + 1) * 1024],
            X.at[r * 128:(r + 1) * 128, pl.ds(pl.multiple_of(half + i * 1024, 1024), 1024)],
            at(yy, x + 1 + 2 * i, z, c),
        )

    def send_diagonal():
        a, b = quarter(6, y + 3, 0), quarter(7, y + 1, 1)
        arrive[7] = [b, quarter(7, y + 1, 0)]
        arrive[6] = [a, quarter(6, y + 3, 1)]

    def halves(r, yy):
        rows = slice(r * 128, (r + 1) * 128)
        return [send(OB.at[rows, :], X.at[rows, pl.ds(half, 2048)], at(yy, x, z, c))]

    arrive = {}
    arrive[4] = [send(OP.at[0], X.at[512:640, cols(block)], at(y + 2, x, z, c))]
    arrive[5] = [send(OP.at[1], X.at[640:768, cols(block5)], at(y + 2, x5, z, c))]
    arrive[1] = [quarter(1, y, 0), quarter(1, y, 1)]
    arrive[2] = halves(2, y + 3)
    arrive[3] = halves(3, y + 1)

    def landed(cps):
        for cp in cps:
            cp.wait_recv()

    def forward(r):
        landed(arrive[r])
        where = X.at[r * 128:(r + 1) * 128, pl.ds(half, 2048)]
        return [send(where, where, other)]

    def spread(b, width, dev):
        where = X.at[512:768, cols(b, width)]
        return send(where, where, dev)

    pair = lambda zz: c * 8 + (zz % 4) * 2
    xdev = at(y, x + 2, z, c)
    up_z, dn_z, far_z = at(y, x, z + 1, c), at(y, x, z + 3, c), at(y, x, z + 2, c)
    gather = {}

    def gather_x():
        landed(arrive[4] + arrive[5])
        gather["x"] = [spread(block, 256, xdev)]

    def gather_z():
        landed(gather["x"])
        gather["z"] = [spread(pair(z), 512, up_z), spread(pair(z), 512, dn_z)]
        gather["core"] = [spread(pair(z), 512, other)]

    def gather_far():
        landed(gather["z"])
        gather["far"] = [spread(pair(z + 3), 256, up_z), spread(pair(z + 1) + 1, 256, dn_z)]
        gather["core"] += [spread(pair(z + 1), 512, other), spread(pair(z + 3), 512, other)]

    def gather_end():
        landed(gather["far"])
        gather["core"].append(spread(pair(z + 2), 512, other))

    def gate_up(k, lo, hi):
        rows = slice(CHUNKS[k][0], CHUNKS[k][0] + CHUNKS[k][1])
        hrows = slice(0, CHUNKS[k][1])

        def tile(t, carry):
            o = cols(t)
            g = dot(X[rows, :], Wg[:, o])
            u = dot(X[rows, :], Wu[:, o])
            hid[hrows, o] = (g / (1.0 + jnp.exp(-g)) * u).astype(BF16)
            return carry

        lax.fori_loop(lo, min(hi, 3), tile, 0)
        if hi > 3:
            w = jnp.concatenate([Wg[:, 768:896], Wu[:, 768:896]], axis=1)
            gu = dot(X[rows, :], w)
            g, u = gu[:, :128], gu[:, 128:]
            hid[hrows, 768:896] = (g / (1.0 + jnp.exp(-g)) * u).astype(BF16)

    def down(k, cc):
        row, n = CHUNKS[k][:2]

        def tile(t, carry):
            for zi in range(2):
                for xi in range(2):
                    zz = t * 2 + zi
                    v = dot(hid[0:n, :], Wd[:, cols(zz * 4 + xi * 2 + cc)])
                    part[cc, zz, xi, row:row + n, :] = v.astype(BF16)
            return carry

        lax.fori_loop(0, 2, tile, 0)

    def add(dst, *srcs):
        total = dst[...].astype(F32)
        for s in srcs:
            total = total + s[...].astype(F32)
        dst[...] = total.astype(BF16)

    zp, zm, zf = (z + 1) % 4, (z + 3) % 4, (z + 2) % 4
    mine = part.at[c]
    st = [dict() for _ in CHUNKS]

    def rows_of(k):
        row, n, a, _ = CHUNKS[k]
        mid = row + a
        return slice(row, mid), slice(mid, row + n), slice(mid, mid + (n - a) // 2), slice(mid + (n - a) // 2, row + n)

    def split(k):
        return CHUNKS[k][2] < CHUNKS[k][1]

    def direct(k):
        return CHUNKS[k][3]

    def send_core(k):
        rows = slice(CHUNKS[k][0], CHUNKS[k][0] + CHUNKS[k][1])
        st[k]["d"] = [send(part.at[1 - c, :, :, rows], rD.at[:, :, rows], other)]

    def s0(k):
        landed(st[k]["d"])
        rows = slice(CHUNKS[k][0], CHUNKS[k][0] + CHUNKS[k][1])
        a, b, _, _ = rows_of(k)

        def body(zz, carry):
            for xi in range(2):
                add(mine.at[zz, xi, rows], rD.at[zz, xi, rows])
            return carry

        lax.fori_loop(0, 4, body, 0)
        st[k]["bx"] = [send(mine.at[:, 1 - xh, b], rBx.at[:, b], xdev)] if split(k) else []
        if direct(k):
            st[k]["a2"] = [
                send(mine.at[zf, :, a], rA3.at[:, a], far_z),
                send(mine.at[zp, :, a], rA2.at[0, :, a], up_z), send(mine.at[zm, :, a], rA2.at[1, :, a], dn_z),
            ]
            return
        st[k]["a1"] = [send(mine.at[zf, 0, a], rA1.at[0, a], up_z), send(mine.at[zf, 1, a], rA1.at[1, a], dn_z)]

    def s1(k):
        a, b, lo, hi = rows_of(k)
        if direct(k):
            landed(st[k]["a2"])
            add(mine.at[z, 1 - xh, a], rA2.at[0, 1 - xh, a], rA2.at[1, 1 - xh, a], rA3.at[1 - xh, a])
            st[k]["ax"] = [send(mine.at[z, 1 - xh, a], rAx.at[a], xdev)]
            landed(st[k]["bx"])

            def body(zz, carry):
                add(mine.at[zz, xh, b], rBx.at[zz, b])
                return carry

            lax.fori_loop(0, 4, body, 0)
            st[k]["b2"] = [
                send(mine.at[zf, xh, b], rB3.at[b], far_z),
                send(mine.at[zp, xh, b], rB2.at[0, b], up_z), send(mine.at[zm, xh, b], rB2.at[1, b], dn_z),
            ]
            return
        landed(st[k]["a1"])
        add(mine.at[zp, 0, a], rA1.at[0, a])
        add(mine.at[zm, 1, a], rA1.at[1, a])
        st[k]["a2"] = [send(mine.at[zp, :, a], rA2.at[0, :, a], up_z), send(mine.at[zm, :, a], rA2.at[1, :, a], dn_z)]
        if not split(k):
            return
        landed(st[k]["bx"])

        def body(zz, carry):
            add(mine.at[zz, xh, b], rBx.at[zz, b])
            return carry

        lax.fori_loop(0, 4, body, 0)
        st[k]["b1"] = [send(mine.at[zf, xh, lo], rB1.at[lo], up_z), send(mine.at[zf, xh, hi], rB1.at[hi], dn_z)]

    def s2(k):
        a, b, lo, hi = rows_of(k)
        if split(k):
            landed(st[k]["b1"])
            add(mine.at[zp, xh, lo], rB1.at[lo])
            add(mine.at[zm, xh, hi], rB1.at[hi])
            st[k]["b2"] = [send(mine.at[zp, xh, b], rB2.at[0, b], up_z), send(mine.at[zm, xh, b], rB2.at[1, b], dn_z)]
        landed(st[k]["a2"])
        add(mine.at[z, 1 - xh, a], rA2.at[0, 1 - xh, a], rA2.at[1, 1 - xh, a])
        st[k]["ax"] = [send(mine.at[z, 1 - xh, a], rAx.at[a], xdev)]

    returned = {}

    def s3(k):
        row, n = CHUNKS[k][:2]
        a, b, _, _ = rows_of(k)
        if split(k):
            landed(st[k]["b2"])
            add(mine.at[z, xh, b], rB2.at[0, b], rB2.at[1, b], *([rB3.at[b]] if direct(k) else []))
        landed(st[k]["ax"])
        add(mine.at[z, xh, a], rA2.at[0, xh, a], rA2.at[1, xh, a], rAx.at[a], *([rA3.at[xh, a]] if direct(k) else []))
        for r in range(row // 128, (row + n) // 128):
            rows = slice(r * 128, (r + 1) * 128)
            dy, dx = REL[r]
            if r == 0:
                G[rows, :] = mine[z, xh, rows, :]
                returned[r] = []
            else:
                owner = {"expert": ((y + dy) % 4) * 2 + (xl + dx) % 2, "ffn": f}
                returned[r] = [send(mine.at[z, xh, rows], G.at[rows], owner)]

    def weigh():
        keyt, gatet = keyr[...].T, gater[...].T
        lanes = lax.broadcasted_iota(jnp.int32, (256, 128), 1).astype(F32)
        for r in range(8):
            w = jnp.where(keyt[:, r:r + 1] == lanes, gatet[:, r:r + 1], 0.0)
            hi = w.astype(BF16)
            whi[:, r * 128:(r + 1) * 128] = hi
            wlo[:, r * 128:(r + 1) * 128] = (w - hi.astype(F32)).astype(BF16)

    def combine(lo, hi):
        for r in range(lo, hi):
            landed(returned[r])
        rows = slice(lo * 128, hi * 128)
        return dot(whi[:, rows], G[rows, :]) + dot(wlo[:, rows], G[rows, :])

    loads[1].wait()
    loads[2].wait()
    gate_up(0, 0, 4)
    loads[3].wait()
    down(0, 1 - c)
    send_core(0)
    down(0, c)
    weigh()
    gather_x()
    fwd1 = forward(1)
    s0(0)
    landed(fwd1)
    gate_up(1, 0, 4)
    gather_z()
    down(1, 1 - c)
    send_core(1)
    down(1, c)
    s1(0)
    s0(1)
    fwd2 = forward(2) + forward(3)
    send_diagonal()
    landed(fwd2)
    gate_up(2, 0, 2)
    gather_far()
    gate_up(2, 2, 4)
    s1(1)
    s2(0)
    down(2, 1 - c)
    send_core(2)
    gather_end()
    down(2, c)
    s2(1)
    s0(2)
    landed(gather["core"])
    gate_up(3, 0, 4)
    s1(2)
    down(3, 1 - c)
    send_core(3)
    down(3, c)
    fwd6 = forward(6)
    fwd7 = forward(7)
    s0(3)
    landed(fwd6)
    gate_up(4, 0, 4)
    s3(0)
    s2(2)
    down(4, 1 - c)
    send_core(4)
    s3(1)
    down(4, c)
    s1(3)
    s0(4)
    landed(fwd7)
    gate_up(5, 0, 4)
    s3(2)
    s2(3)
    down(5, 1 - c)
    send_core(5)
    s1(4)
    down(5, c)
    s0(5)
    s3(3)
    mixed[...] = combine(0, 4)
    s1(5)
    s3(4)
    mixed[...] += combine(4, 6)
    s3(5)
    out_ref[...] = (mixed[...] + combine(6, 8)).astype(BF16)
    for cp in copies:
        cp.wait_send()


N_COPIES = 110


def per_device(tokens, router_gates, routes, gate_proj, up_proj, down_proj):
    rows, width = tokens.shape
    hidden = gate_proj.shape[2]
    vmem = lambda *shape: pltpu.VMEM(shape, BF16)
    any_spec = pl.BlockSpec(memory_space=pl.ANY)
    vmem_spec = pl.BlockSpec(memory_space=pltpu.VMEM)
    return pl.pallas_call(
        kernel,
        out_shape=jax.ShapeDtypeStruct((rows, 256), BF16),
        in_specs=[any_spec, vmem_spec, vmem_spec, any_spec, any_spec, any_spec],
        out_specs=vmem_spec,
        scratch_shapes=[
            vmem(1024, width), vmem(width, hidden), vmem(width, hidden), vmem(hidden, width),
            vmem(rows, width), vmem(1024, 2048), vmem(2, 128, 256), vmem(256, hidden),
            vmem(2, 4, 2, 1024, 256), vmem(4, 2, 1024, 256),
            vmem(2, 1024, 256), vmem(2, 2, 1024, 256), vmem(1024, 256),
            vmem(4, 1024, 256), vmem(1024, 256), vmem(2, 1024, 256), vmem(2, 1024, 256), vmem(1024, 256), vmem(1024, 256),
            vmem(1024, 256), vmem(256, 1024), vmem(256, 1024),
            pltpu.VMEM((2, 8, 256), F32), pltpu.VMEM((8, 256), F32), pltpu.VMEM((8, 256), F32),
            pltpu.VMEM((256, 256), F32),
            pltpu.SemaphoreType.DMA((N_COPIES,)), pltpu.SemaphoreType.DMA((N_COPIES,)),
            pltpu.SemaphoreType.DMA((4,)),
        ],
        compiler_params=pltpu.CompilerParams(
            collective_id=0, has_side_effects=True, vmem_limit_bytes=67043328
        ),
        name="layer",
    )(tokens, routes.T, router_gates.T, gate_proj[0], up_proj[0], down_proj[0])


def solution(mesh):
    in_specs = (
        P("expert", None),
        P("expert", None),
        P("expert", None),
        P("expert", None, "ffn"),
        P("expert", None, "ffn"),
        P("expert", "ffn", None),
    )
    out_specs = P("expert", "ffn")
    return jax.shard_map(
        per_device, mesh=mesh, in_specs=in_specs, out_specs=out_specs, check_vma=False
    )
```

```python
import jax
import jax.numpy as jnp
from jax import lax
from jax.experimental import pallas as pl
from jax.experimental.pallas import tpu as pltpu
from jax.sharding import PartitionSpec as P

MESH = pl.DeviceIdType.MESH
REL = ((0, 0), (0, 1), (1, 0), (3, 0), (2, 1), (1, 1), (3, 1), (2, 0))
CHUNKS = (
    (0, 128, 96, False), (128, 128, 128, False), (256, 128, 128, False), (384, 128, 128, False),
    (512, 128, 96, False), (640, 128, 64, True), (768, 128, 64, True), (896, 128, 64, True),
)
F32 = jnp.float32
BF16 = jnp.bfloat16


def dot(a, b):
    return jnp.dot(a, b, preferred_element_type=F32)


def kernel(
    tok_hbm, routes_hbm, gates_hbm, gate_hbm, up_hbm, down_hbm, out_ref,
    X, Wg, Wu, Wd, tok, OB, OP, hid, part, rD, rA1, rA2, rAx, rBx, rB1, rB2, G,
    placing, whi, wlo, keys, keyr, gater, mixed, routes, gates,
    send_sem, recv_sem, local_sem,
):
    e = lax.axis_index("expert")
    f = lax.axis_index("ffn")
    y, xl = e // 2, e % 2
    z, xh, c = f // 4, (f // 2) % 2, f % 2
    x = xh * 2 + xl

    def at(yy, xx, zz, cc):
        yy, xx, zz = yy % 4, xx % 4, zz % 4
        return {"expert": yy * 2 + xx % 2, "ffn": zz * 4 + (xx // 2) * 2 + cc}

    loads = [
        pltpu.make_async_copy(s, d, local_sem.at[i])
        for i, (s, d) in enumerate((
            (tok_hbm, tok), (gate_hbm, Wg), (up_hbm, Wu), (down_hbm, Wd), (routes_hbm, routes), (gates_hbm, gates),
        ))
    ]
    for i in (4, 5, 0):
        loads[i].start()

    barrier = pltpu.get_barrier_semaphore()
    peers = [
        at(y, x, z, 1 - c), at(y, x + 1, z, c), at(y, x + 3, z, c), at(y, x + 2, z, c),
        at(y + 1, x, z, c), at(y + 3, x, z, c), at(y + 2, x, z, c),
        at(y + 1, x + 1, z, c), at(y + 1, x + 3, z, c), at(y + 3, x + 1, z, c), at(y + 3, x + 3, z, c),
        at(y + 2, x + 1, z, c), at(y + 2, x + 3, z, c), at(y, x, z + 1, c), at(y, x, z + 3, c),
        at(y, x, z + 2, c),
    ]
    for dev in peers:
        pl.semaphore_signal(barrier, inc=1, device_id=dev, device_id_type=MESH)

    loads[4].wait()
    loads[5].wait()
    expert_ids = lax.broadcasted_iota(jnp.int32, (8, 256), 0)
    first, second = routes[0:1, :] == expert_ids, routes[1:2, :] == expert_ids
    chosen = jnp.where(first | second, 1.0, 0.0)
    earlier = lax.broadcasted_iota(jnp.int32, (256, 256), 0) < lax.broadcasted_iota(jnp.int32, (256, 256), 1)
    rank = dot(chosen.astype(BF16), jnp.where(earlier, 1.0, 0.0).astype(BF16))
    keys[0] = jnp.where(first | second, rank, -1.0)
    keys[1] = jnp.where(first, gates[0:1, :], 0.0) + jnp.where(second, gates[1:2, :], 0.0)
    row_ids = lax.broadcasted_iota(jnp.int32, (128, 256), 0).astype(F32)
    for r, (dy, dx) in enumerate(REL):
        owner = ((y + 4 - dy) % 4) * 2 + (xl + dx) % 2
        key = keys[0, pl.ds(owner, 1), :]
        keyr[r:r + 1, :] = key
        gater[r:r + 1, :] = keys[1, pl.ds(owner, 1), :]
        placing[r * 128:(r + 1) * 128, :] = jnp.where(key == row_ids, 1.0, 0.0).astype(BF16)

    copies = []
    slots = {}

    def send(src, dst, dev, key):
        i = len(copies)
        if i >= N_SEND:
            copies[i - N_SEND].wait_send()
        cp = pltpu.make_async_remote_copy(
            src_ref=src, dst_ref=dst, send_sem=send_sem.at[i % N_SEND],
            recv_sem=recv_sem.at[slots.setdefault(key, len(slots))], device_id=dev, device_id_type=MESH,
        )
        cp.start()
        copies.append(cp)

    def got(key, where):
        pltpu.make_async_copy(where, where, recv_sem.at[slots[key]]).wait()

    other = at(y, x, z, 1 - c)
    half = pl.multiple_of(c * 2048, 2048)

    def cols(b, width=256):
        return pl.ds(pl.multiple_of(b * 256, 256), width)

    x4 = (x + 1 + 2 * c) % 4
    block = c * 8 + z * 2 + xh
    block4 = c * 8 + z * 2 + x4 // 2
    loads[0].wait()
    loads[1].start()
    loads[2].start()
    OP[...] = dot(placing[512:640, :], tok[:, cols(block4)]).astype(BF16)

    def place(lo, hi, to):
        def tile(t, carry):
            o = pl.multiple_of(t * 1024, 1024)
            v = dot(placing[lo:hi, :], tok[:, pl.ds(pl.multiple_of(half + o, 1024), 1024)])
            OB[to:to + hi - lo, pl.ds(o, 1024)] = v.astype(BF16)
            return carry

        lax.fori_loop(0, 2, tile, 0)

    def place_own(t, carry):
        o = pl.ds(pl.multiple_of(t * 1024, 1024), 1024)
        X[0:128, o] = dot(placing[0:128, :], tok[:, o]).astype(BF16)
        return carry

    outbox = {1: 0, 2: 128, 3: 256, 5: 384, 6: 512, 7: 640}
    place(128, 256, outbox[1])
    pl.semaphore_wait(barrier, len(peers))

    def quarter(r, yy, i):
        return send(
            OB.at[outbox[r]:outbox[r] + 128, i * 1024:(i + 1) * 1024],
            X.at[r * 128:(r + 1) * 128, pl.ds(pl.multiple_of(half + i * 1024, 1024), 1024)],
            at(yy, x + 1 + 2 * i, z, c), r,
        )

    def halves(r, yy):
        rows = slice(r * 128, (r + 1) * 128)
        send(OB.at[outbox[r]:outbox[r] + 128, :], X.at[rows, pl.ds(half, 2048)], at(yy, x, z, c), r)

    def send_diagonal():
        for r, yy, i in ((5, y + 3, 0), (6, y + 1, 1), (6, y + 1, 0), (5, y + 3, 1)):
            quarter(r, yy, i)

    send(OP, X.at[512:640, cols(block4)], at(y + 2, x4, z, c), 4)
    quarter(1, y, 0)
    quarter(1, y, 1)
    place(256, 512, outbox[2])
    halves(2, y + 3)
    halves(3, y + 1)
    loads[3].start()
    place(640, 1024, outbox[5])
    lax.fori_loop(0, 4, place_own, 0)

    def half_rows(lo, hi):
        return X.at[lo * 128:hi * 128, pl.ds(half, 2048)]

    def forward(lo, hi):
        for r in range(lo, hi):
            got(r, half_rows(r, r + 1))
        send(half_rows(lo, hi), half_rows(lo, hi), other, ("core", lo))

    def forwarded(lo, hi):
        got(("core", lo), half_rows(lo, hi))

    def spread(b, width, dev, key):
        where = X.at[512:640, cols(b, width)]
        send(where, where, dev, key)

    pair = lambda zz: c * 8 + (zz % 4) * 2
    xdev = at(y, x + 2, z, c)
    up_z, dn_z, far_z = at(y, x, z + 1, c), at(y, x, z + 3, c), at(y, x, z + 2, c)

    def gather_x():
        got(4, OP)
        spread(block, 256, xdev, "x")

    def gather_z():
        got("x", X.at[512:640, 0:256])
        spread(pair(z), 512, up_z, "z")
        spread(pair(z), 512, dn_z, "z")
        spread(pair(z), 512, other, "c")

    def gather_far():
        got("z", X.at[512:640, 0:1024])
        spread(pair(z + 3), 256, up_z, "far")
        spread(pair(z + 1) + 1, 256, dn_z, "far")
        spread(pair(z + 1), 512, other, "c")
        spread(pair(z + 3), 512, other, "c")

    def gather_end():
        got("far", X.at[512:640, 0:512])
        spread(pair(z + 2), 512, other, "c")

    def gathered():
        got("c", half_rows(4, 5))

    def gate_up(k, lo, hi):
        rows = slice(CHUNKS[k][0], CHUNKS[k][0] + CHUNKS[k][1])
        hrows = slice(0, CHUNKS[k][1])

        def tile(t, carry):
            o = cols(t)
            g = dot(X[rows, :], Wg[:, o])
            u = dot(X[rows, :], Wu[:, o])
            hid[hrows, o] = (g / (1.0 + jnp.exp(-g)) * u).astype(BF16)
            return carry

        lax.fori_loop(lo, min(hi, 3), tile, 0)
        if hi > 3:
            w = jnp.concatenate([Wg[:, 768:896], Wu[:, 768:896]], axis=1)
            gu = dot(X[rows, :], w)
            g, u = gu[:, :128], gu[:, 128:]
            hid[hrows, 768:896] = (g / (1.0 + jnp.exp(-g)) * u).astype(BF16)

    def down(k, cc):
        row, n = CHUNKS[k][:2]

        def tile(t, carry):
            for zi in range(2):
                for xi in range(2):
                    zz = t * 2 + zi
                    v = dot(hid[0:n, :], Wd[:, cols(zz * 4 + xi * 2 + cc)])
                    part[cc, zz, xi, row:row + n, :] = v.astype(BF16)
            return carry

        lax.fori_loop(0, 2, tile, 0)

    def down_other(k):
        rows = slice(CHUNKS[k][0], CHUNKS[k][0] + CHUNKS[k][1])
        down(k, 1 - c)
        send(part.at[1 - c, :, :, rows], rD.at[:, :, rows], other, ("d", k))

    def down_own(k):
        down(k, c)

    def add(dst, *srcs):
        total = dst[...].astype(F32)
        for s in srcs:
            total = total + s[...].astype(F32)
        dst[...] = total.astype(BF16)

    zp, zm, zf = (z + 1) % 4, (z + 3) % 4, (z + 2) % 4
    mine = part.at[c]

    def rows_of(k):
        row, n, a, _ = CHUNKS[k]
        mid = row + a
        return slice(row, mid), slice(mid, row + n), slice(mid, mid + (n - a) // 2), slice(mid + (n - a) // 2, row + n)

    def split(k):
        return CHUNKS[k][2] < CHUNKS[k][1]

    def direct(k):
        return CHUNKS[k][3]

    def s0(k):
        rows = slice(CHUNKS[k][0], CHUNKS[k][0] + CHUNKS[k][1])
        got(("d", k), rD.at[:, :, rows])
        a, b, _, _ = rows_of(k)

        def body(zz, carry):
            for xi in range(2):
                add(mine.at[zz, xi, rows], rD.at[zz, xi, rows])
            return carry

        lax.fori_loop(0, 4, body, 0)
        if split(k):
            send(mine.at[:, 1 - xh, b], rBx.at[:, b], xdev, ("bx", k))
        if direct(k):
            send(mine.at[zf, :, a], rA2.at[2, :, a], far_z, ("a2", k))
            send(mine.at[zp, :, a], rA2.at[0, :, a], up_z, ("a2", k))
            send(mine.at[zm, :, a], rA2.at[1, :, a], dn_z, ("a2", k))
        else:
            send(mine.at[zf, 0, a], rA1.at[0, a], up_z, ("a1", k))
            send(mine.at[zf, 1, a], rA1.at[1, a], dn_z, ("a1", k))

    def z_terms(k):
        return range(3 if direct(k) else 2)

    def x_first(k):
        _, b, lo, hi = rows_of(k)
        got(("bx", k), rBx.at[:, b])

        def body(zz, carry):
            add(mine.at[zz, xh, b], rBx.at[zz, b])
            return carry

        lax.fori_loop(0, 4, body, 0)
        if direct(k):
            send(mine.at[zf, xh, b], rB2.at[2, b], far_z, ("b2", k))
            send(mine.at[zp, xh, b], rB2.at[0, b], up_z, ("b2", k))
            send(mine.at[zm, xh, b], rB2.at[1, b], dn_z, ("b2", k))
        else:
            send(mine.at[zf, xh, lo], rB1.at[lo], up_z, ("b1", k))
            send(mine.at[zf, xh, hi], rB1.at[hi], dn_z, ("b1", k))

    def z_sum(k):
        a = rows_of(k)[0]
        got(("a2", k), rA2.at[0:len(z_terms(k)), :, a])
        add(mine.at[z, 1 - xh, a], *[rA2.at[i, 1 - xh, a] for i in z_terms(k)])
        send(mine.at[z, 1 - xh, a], rAx.at[a], xdev, ("ax", k))

    def s1(k):
        a = rows_of(k)[0]
        if direct(k):
            z_sum(k)
        else:
            got(("a1", k), rA1.at[:, a])
            add(mine.at[zp, 0, a], rA1.at[0, a])
            add(mine.at[zm, 1, a], rA1.at[1, a])
            send(mine.at[zp, :, a], rA2.at[0, :, a], up_z, ("a2", k))
            send(mine.at[zm, :, a], rA2.at[1, :, a], dn_z, ("a2", k))
        if split(k):
            x_first(k)

    def s2(k):
        _, b, lo, hi = rows_of(k)
        if split(k):
            got(("b1", k), rB1.at[b])
            add(mine.at[zp, xh, lo], rB1.at[lo])
            add(mine.at[zm, xh, hi], rB1.at[hi])
            send(mine.at[zp, xh, b], rB2.at[0, b], up_z, ("b2", k))
            send(mine.at[zm, xh, b], rB2.at[1, b], dn_z, ("b2", k))
        z_sum(k)

    def s3(k):
        row, n = CHUNKS[k][:2]
        a, b, _, _ = rows_of(k)
        if split(k):
            got(("b2", k), rB2.at[0:len(z_terms(k)), b])
            add(mine.at[z, xh, b], *[rB2.at[i, b] for i in z_terms(k)])
        got(("ax", k), rAx.at[a])
        add(mine.at[z, xh, a], rAx.at[a], *[rA2.at[i, xh, a] for i in z_terms(k)])
        for r in range(row // 128, (row + n) // 128):
            rows = slice(r * 128, (r + 1) * 128)
            dy, dx = REL[r]
            if r == 0:
                G[rows, :] = mine[z, xh, rows, :]
            else:
                owner = {"expert": ((y + dy) % 4) * 2 + (xl + dx) % 2, "ffn": f}
                send(mine.at[z, xh, rows], G.at[rows], owner, ("back", k))

    def weigh():
        keyt, gatet = keyr[...].T, gater[...].T
        lanes = lax.broadcasted_iota(jnp.int32, (256, 128), 1).astype(F32)
        for r in range(8):
            w = jnp.where(keyt[:, r:r + 1] == lanes, gatet[:, r:r + 1], 0.0)
            hi = w.astype(BF16)
            whi[:, r * 128:(r + 1) * 128] = hi
            wlo[:, r * 128:(r + 1) * 128] = (w - hi.astype(F32)).astype(BF16)

    def combine(k):
        rows = slice(CHUNKS[k][0], CHUNKS[k][0] + CHUNKS[k][1])
        if k:
            got(("back", k), G.at[rows])
        return dot(whi[:, rows], G[rows, :]) + dot(wlo[:, rows], G[rows, :])

    loads[1].wait()
    loads[2].wait()
    gate_up(0, 0, 4)
    loads[3].wait()
    down_other(0)
    down_own(0)
    weigh()
    gather_x()
    forward(1, 2)
    s0(0)
    forwarded(1, 2)
    gate_up(1, 0, 4)
    gather_z()
    down_other(1)
    down_own(1)
    forward(2, 3)
    forward(3, 4)
    send_diagonal()
    s0(1)
    forwarded(2, 3)
    gate_up(2, 0, 2)
    s1(0)
    gate_up(2, 2, 4)
    gather_far()
    down_other(2)
    down_own(2)
    forwarded(3, 4)
    gate_up(3, 0, 2)
    s0(2)
    s1(1)
    gate_up(3, 2, 4)
    gather_end()
    down_other(3)
    s2(0)
    halves(7, y + 2)
    down_own(3)
    gathered()
    gate_up(4, 0, 2)
    s0(3)
    s1(2)
    gate_up(4, 2, 4)
    down_other(4)
    s2(1)
    forward(5, 7)
    down_own(4)
    forwarded(5, 7)
    gate_up(5, 0, 2)
    s0(4)
    s1(3)
    gate_up(5, 2, 4)
    down_other(5)
    s2(2)
    s3(0)
    down_own(5)
    gate_up(6, 0, 2)
    s0(5)
    s1(4)
    gate_up(6, 2, 4)
    down_other(6)
    s2(3)
    s3(1)
    forward(7, 8)
    down_own(6)
    forwarded(7, 8)
    gate_up(7, 0, 2)
    s0(6)
    gate_up(7, 2, 4)
    s1(5)
    down_other(7)
    s2(4)
    s3(2)
    down_own(7)
    s0(7)
    s3(3)
    mixed[...] = combine(0) + combine(1) + combine(2)
    s1(6)
    s3(4)
    s3(5)
    s1(7)
    s3(6)
    mixed[...] += combine(3) + combine(4)
    s3(7)
    mixed[...] += combine(5) + combine(6)
    out_ref[...] = (mixed[...] + combine(7)).astype(BF16)
    assert len(slots) == N_RECV
    for cp in copies[-N_SEND:]:
        cp.wait_send()


N_SEND = 20
N_RECV = 64


def per_device(tokens, router_gates, routes, gate_proj, up_proj, down_proj):
    rows, width = tokens.shape
    hidden = gate_proj.shape[2]
    vmem = lambda *shape: pltpu.VMEM(shape, BF16)
    return pl.pallas_call(
        kernel,
        out_shape=jax.ShapeDtypeStruct((rows, 256), BF16),
        in_specs=[pl.BlockSpec(memory_space=pltpu.HBM)] * 6,
        out_specs=pl.BlockSpec(memory_space=pltpu.VMEM),
        scratch_shapes=[
            vmem(1024, width), vmem(width, hidden), vmem(width, hidden), vmem(hidden, width),
            vmem(rows, width), vmem(768, 2048), vmem(128, 256), vmem(256, hidden),
            vmem(2, 4, 2, 1024, 256), vmem(4, 2, 1024, 256),
            vmem(2, 1024, 256), vmem(3, 2, 1024, 256), vmem(1024, 256),
            vmem(4, 1024, 256), vmem(1024, 256), vmem(3, 1024, 256), vmem(1024, 256),
            vmem(1024, 256), vmem(256, 1024), vmem(256, 1024),
            pltpu.VMEM((2, 8, 256), F32), pltpu.VMEM((8, 256), F32), pltpu.VMEM((8, 256), F32),
            pltpu.VMEM((256, 256), F32), pltpu.VMEM((2, 256), jnp.int32), pltpu.VMEM((2, 256), F32),
            pltpu.SemaphoreType.DMA((N_SEND,)), pltpu.SemaphoreType.DMA((N_RECV,)),
            pltpu.SemaphoreType.DMA((6,)),
        ],
        compiler_params=pltpu.CompilerParams(
            collective_id=0, has_side_effects=True, vmem_limit_bytes=66 * 10**6
        ),
        name="layer",
    )(tokens, routes.T, router_gates.T, gate_proj[0], up_proj[0], down_proj[0])


def solution(mesh):
    in_specs = (
        P("expert", None),
        P("expert", None),
        P("expert", None),
        P("expert", None, "ffn"),
        P("expert", None, "ffn"),
        P("expert", "ffn", None),
    )
    out_specs = P("expert", "ffn")
    return jax.shard_map(
        per_device, mesh=mesh, in_specs=in_specs, out_specs=out_specs, check_vma=False
    )
```

```python
import jax
import jax.numpy as jnp
from jax import lax
from jax.experimental import pallas as pl
from jax.experimental.pallas import tpu as pltpu
from jax.sharding import PartitionSpec as P

MESH = pl.DeviceIdType.MESH
REL = ((0, 0), (0, 1), (1, 0), (3, 0), (2, 1), (2, 0), (1, 1), (3, 1))
CHUNKS = (
    (0, 128, 96, False), (128, 128, 128, False), (256, 128, 128, False), (384, 128, 128, False),
    (512, 128, 64, False), (768, 128, 48, True), (896, 128, 64, True), (640, 128, 64, True),
)
F32 = jnp.float32
BF16 = jnp.bfloat16


def dot(a, b):
    return jnp.dot(a, b, preferred_element_type=F32)


def kernel(
    tok_hbm, routes_hbm, gates_hbm, gate_hbm, up_hbm, down_hbm, out_ref,
    X, Wg, Wu, Wd, tok, OB, OP, hid, part, rD, rA1, rA2, rAx, rBx, rB1, rB2, G,
    placing, whi, wlo, keys, keyr, gater, mixed, routes, gates,
    send_sem, recv_sem, local_sem,
):
    e = lax.axis_index("expert")
    f = lax.axis_index("ffn")
    y, xl = e // 2, e % 2
    z, xh, c = f // 4, (f // 2) % 2, f % 2
    x = xh * 2 + xl

    def at(yy, xx, zz, cc):
        yy, xx, zz = yy % 4, xx % 4, zz % 4
        return {"expert": yy * 2 + xx % 2, "ffn": zz * 4 + (xx // 2) * 2 + cc}

    loads = [
        pltpu.make_async_copy(s, d, local_sem.at[i])
        for i, (s, d) in enumerate((
            (tok_hbm, tok), (gate_hbm, Wg), (up_hbm, Wu), (down_hbm, Wd), (routes_hbm, routes), (gates_hbm, gates),
        ))
    ]
    for i in (4, 5, 0):
        loads[i].start()

    barrier = pltpu.get_barrier_semaphore()
    peers = [
        at(y, x, z, 1 - c), at(y, x + 1, z, c), at(y, x + 3, z, c), at(y, x + 2, z, c),
        at(y + 1, x, z, c), at(y + 3, x, z, c), at(y + 2, x, z, c),
        at(y + 1, x + 1, z, c), at(y + 1, x + 3, z, c), at(y + 3, x + 1, z, c), at(y + 3, x + 3, z, c),
        at(y + 2, x + 1, z, c), at(y + 2, x + 3, z, c), at(y, x, z + 1, c), at(y, x, z + 3, c),
        at(y, x, z + 2, c),
    ]
    for dev in peers:
        pl.semaphore_signal(barrier, inc=1, device_id=dev, device_id_type=MESH)

    loads[4].wait()
    loads[5].wait()
    expert_ids = lax.broadcasted_iota(jnp.int32, (8, 256), 0)
    first, second = routes[0:1, :] == expert_ids, routes[1:2, :] == expert_ids
    chosen = jnp.where(first | second, 1.0, 0.0)
    earlier = lax.broadcasted_iota(jnp.int32, (256, 256), 0) < lax.broadcasted_iota(jnp.int32, (256, 256), 1)
    rank = dot(chosen.astype(BF16), jnp.where(earlier, 1.0, 0.0).astype(BF16))
    keys[0] = jnp.where(first | second, rank, -1.0)
    keys[1] = jnp.where(first, gates[0:1, :], 0.0) + jnp.where(second, gates[1:2, :], 0.0)
    row_ids = lax.broadcasted_iota(jnp.int32, (128, 256), 0).astype(F32)
    for r, (dy, dx) in enumerate(REL):
        owner = ((y + 4 - dy) % 4) * 2 + (xl + dx) % 2
        key = keys[0, pl.ds(owner, 1), :]
        keyr[r:r + 1, :] = key
        gater[r:r + 1, :] = keys[1, pl.ds(owner, 1), :]
        placing[r * 128:(r + 1) * 128, :] = jnp.where(key == row_ids, 1.0, 0.0).astype(BF16)

    copies = []
    slots = {}

    def send(src, dst, dev, key):
        i = len(copies)
        if i >= N_SEND:
            copies[i - N_SEND].wait_send()
        cp = pltpu.make_async_remote_copy(
            src_ref=src, dst_ref=dst, send_sem=send_sem.at[i % N_SEND],
            recv_sem=recv_sem.at[slots.setdefault(key, len(slots))], device_id=dev, device_id_type=MESH,
        )
        cp.start()
        copies.append(cp)

    def got(key, where):
        pltpu.make_async_copy(where, where, recv_sem.at[slots[key]]).wait()

    other = at(y, x, z, 1 - c)
    half = pl.multiple_of(c * 2048, 2048)

    def cols(b, width=256):
        return pl.ds(pl.multiple_of(b * 256, 256), width)

    x4 = (x + 1 + 2 * c) % 4
    block = c * 8 + z * 2 + xh
    block4 = c * 8 + z * 2 + x4 // 2
    loads[0].wait()
    loads[1].start()
    loads[2].start()
    OP[0:128, :] = dot(placing[512:640, :], tok[:, cols(block4)]).astype(BF16)
    OP[128:192, :] = dot(placing[640:704, :], tok[:, cols(block)]).astype(BF16)

    def place(lo, hi, to):
        def tile(t, carry):
            o = pl.multiple_of(t * 1024, 1024)
            v = dot(placing[lo:hi, :], tok[:, pl.ds(pl.multiple_of(half + o, 1024), 1024)])
            OB[to:to + hi - lo, pl.ds(o, 1024)] = v.astype(BF16)
            return carry

        lax.fori_loop(0, 2, tile, 0)

    def place_own(t, carry):
        o = pl.ds(pl.multiple_of(t * 1024, 1024), 1024)
        X[0:128, o] = dot(placing[0:128, :], tok[:, o]).astype(BF16)
        return carry

    outbox = {1: 0, 2: 128, 3: 256, 6: 448, 7: 576}
    place(128, 256, outbox[1])
    pl.semaphore_wait(barrier, len(peers))

    def quarter(r, yy, i):
        return send(
            OB.at[outbox[r]:outbox[r] + 128, i * 1024:(i + 1) * 1024],
            X.at[r * 128:(r + 1) * 128, pl.ds(pl.multiple_of(half + i * 1024, 1024), 1024)],
            at(yy, x + 1 + 2 * i, z, c), r,
        )

    def halves(r, yy):
        rows = slice(r * 128, (r + 1) * 128)
        send(OB.at[outbox[r]:outbox[r] + 128, :], X.at[rows, pl.ds(half, 2048)], at(yy, x, z, c), r)

    def send_diagonal():
        for r, yy, i in ((6, y + 3, 0), (7, y + 1, 1), (7, y + 1, 0), (6, y + 3, 1)):
            quarter(r, yy, i)

    send(OP.at[0:128], X.at[512:640, cols(block4)], at(y + 2, x4, z, c), 4)
    send(OP.at[128:192], X.at[640:704, cols(block)], at(y + 2, x, z, c), 5)
    quarter(1, y, 0)
    quarter(1, y, 1)
    place(256, 512, outbox[2])
    halves(2, y + 3)
    halves(3, y + 1)
    loads[3].start()
    place(704, 1024, 384)
    lax.fori_loop(0, 4, place_own, 0)

    def half_rows(lo, hi):
        return X.at[lo * 128:hi * 128, pl.ds(half, 2048)]

    def forward(r):
        got(r, half_rows(r, r + 1))
        send(half_rows(r, r + 1), half_rows(r, r + 1), other, ("core", r))

    def forwarded(r):
        got(("core", r), half_rows(r, r + 1))

    last = X.at[704:768, pl.ds(half, 2048)]

    def send_last():
        send(OB.at[384:448, :], last, at(y + 2, x, z, c), "last")

    def forward_last():
        got("last", last)
        send(last, last, other, ("core", 5))

    def forwarded_last():
        got(("core", 5), last)

    def spread(b, width, dev, key):
        where = X.at[512:704, cols(b, width)]
        send(where, where, dev, key)

    pair = lambda zz: c * 8 + (zz % 4) * 2
    xdev = at(y, x + 2, z, c)
    up_z, dn_z, far_z = at(y, x, z + 1, c), at(y, x, z + 3, c), at(y, x, z + 2, c)

    def gather_x():
        got(4, OP.at[0:128])
        got(5, OP.at[128:192])
        spread(block, 256, xdev, "x")

    def gather_z():
        got("x", X.at[512:704, 0:256])
        spread(pair(z), 512, up_z, "z")
        spread(pair(z), 512, dn_z, "z")
        spread(pair(z), 512, other, "c")

    def gather_far():
        got("z", X.at[512:704, 0:1024])
        spread(pair(z + 3), 256, up_z, "far")
        spread(pair(z + 1) + 1, 256, dn_z, "far")
        spread(pair(z + 1), 512, other, "c")
        spread(pair(z + 3), 512, other, "c")

    def gather_end():
        got("far", X.at[512:704, 0:512])
        spread(pair(z + 2), 512, other, "c")

    def gathered():
        got("c", X.at[512:704, pl.ds(half, 2048)])

    def gate_up(k, lo, hi):
        row, n = CHUNKS[k][:2]
        w = jnp.concatenate([Wg[:, lo:hi], Wu[:, lo:hi]], axis=1)
        both = dot(X[row:row + n, :], w)
        g, u = both[:, :hi - lo], both[:, hi - lo:]
        hid[0:n, lo:hi] = (g / (1.0 + jnp.exp(-g)) * u).astype(BF16)

    def down(k, cc):
        row, n = CHUNKS[k][:2]
        w = jnp.concatenate([Wd[:, cols(b * 2 + cc)] for b in range(8)], axis=1)
        v = dot(hid[0:n, :], w).astype(BF16)
        for b in range(8):
            part[cc, b // 2, b % 2, row:row + n, :] = v[:, b * 256:(b + 1) * 256]

    def down_other(k):
        rows = slice(CHUNKS[k][0], CHUNKS[k][0] + CHUNKS[k][1])
        down(k, 1 - c)
        send(part.at[1 - c, :, :, rows], rD.at[:, :, rows], other, ("d", k))

    def down_own(k):
        down(k, c)

    def add(dst, *srcs):
        total = dst[...].astype(F32)
        for s in srcs:
            total = total + s[...].astype(F32)
        dst[...] = total.astype(BF16)

    zp, zm, zf = (z + 1) % 4, (z + 3) % 4, (z + 2) % 4
    mine = part.at[c]

    def rows_of(k):
        row, n, a, _ = CHUNKS[k]
        mid = row + a
        return slice(row, mid), slice(mid, row + n), slice(mid, mid + (n - a) // 2), slice(mid + (n - a) // 2, row + n)

    def split(k):
        return CHUNKS[k][2] < CHUNKS[k][1]

    def direct(k):
        return CHUNKS[k][3]

    def s0(k):
        rows = slice(CHUNKS[k][0], CHUNKS[k][0] + CHUNKS[k][1])
        got(("d", k), rD.at[:, :, rows])
        a, b, _, _ = rows_of(k)

        def body(zz, carry):
            for xi in range(2):
                add(mine.at[zz, xi, rows], rD.at[zz, xi, rows])
            return carry

        lax.fori_loop(0, 4, body, 0)
        if split(k):
            send(mine.at[:, 1 - xh, b], rBx.at[:, b], xdev, ("bx", k))
        if direct(k):
            send(mine.at[zf, :, a], rA2.at[2, :, a], far_z, ("a2", k))
            send(mine.at[zp, :, a], rA2.at[0, :, a], up_z, ("a2", k))
            send(mine.at[zm, :, a], rA2.at[1, :, a], dn_z, ("a2", k))
        else:
            send(mine.at[zf, 0, a], rA1.at[0, a], up_z, ("a1", k))
            send(mine.at[zf, 1, a], rA1.at[1, a], dn_z, ("a1", k))

    def z_terms(k):
        return range(3 if direct(k) else 2)

    def x_first(k):
        _, b, lo, hi = rows_of(k)
        got(("bx", k), rBx.at[:, b])

        def body(zz, carry):
            add(mine.at[zz, xh, b], rBx.at[zz, b])
            return carry

        lax.fori_loop(0, 4, body, 0)
        if direct(k):
            send(mine.at[zf, xh, b], rB2.at[2, b], far_z, ("b2", k))
            send(mine.at[zp, xh, b], rB2.at[0, b], up_z, ("b2", k))
            send(mine.at[zm, xh, b], rB2.at[1, b], dn_z, ("b2", k))
        else:
            send(mine.at[zf, xh, lo], rB1.at[lo], up_z, ("b1", k))
            send(mine.at[zf, xh, hi], rB1.at[hi], dn_z, ("b1", k))

    def z_sum(k):
        a = rows_of(k)[0]
        got(("a2", k), rA2.at[0:len(z_terms(k)), :, a])
        add(mine.at[z, 1 - xh, a], *[rA2.at[i, 1 - xh, a] for i in z_terms(k)])
        send(mine.at[z, 1 - xh, a], rAx.at[a], xdev, ("ax", k))

    def s1(k):
        a = rows_of(k)[0]
        if direct(k):
            z_sum(k)
        else:
            got(("a1", k), rA1.at[:, a])
            add(mine.at[zp, 0, a], rA1.at[0, a])
            add(mine.at[zm, 1, a], rA1.at[1, a])
            send(mine.at[zp, :, a], rA2.at[0, :, a], up_z, ("a2", k))
            send(mine.at[zm, :, a], rA2.at[1, :, a], dn_z, ("a2", k))
        if split(k):
            x_first(k)

    def s2(k):
        _, b, lo, hi = rows_of(k)
        if split(k):
            got(("b1", k), rB1.at[b])
            add(mine.at[zp, xh, lo], rB1.at[lo])
            add(mine.at[zm, xh, hi], rB1.at[hi])
            send(mine.at[zp, xh, b], rB2.at[0, b], up_z, ("b2", k))
            send(mine.at[zm, xh, b], rB2.at[1, b], dn_z, ("b2", k))
        z_sum(k)

    def s3(k):
        row, n = CHUNKS[k][:2]
        a, b, _, _ = rows_of(k)
        if split(k):
            got(("b2", k), rB2.at[0:len(z_terms(k)), b])
            add(mine.at[z, xh, b], *[rB2.at[i, b] for i in z_terms(k)])
        got(("ax", k), rAx.at[a])
        add(mine.at[z, xh, a], rAx.at[a], *[rA2.at[i, xh, a] for i in z_terms(k)])
        for r in range(row // 128, (row + n) // 128):
            rows = slice(r * 128, (r + 1) * 128)
            dy, dx = REL[r]
            if r == 0:
                G[rows, :] = mine[z, xh, rows, :]
            else:
                owner = {"expert": ((y + dy) % 4) * 2 + (xl + dx) % 2, "ffn": f}
                send(mine.at[z, xh, rows], G.at[rows], owner, ("back", k))

    def weigh():
        keyt, gatet = keyr[...].T, gater[...].T
        lanes = lax.broadcasted_iota(jnp.int32, (256, 128), 1).astype(F32)
        for r in range(8):
            w = jnp.where(keyt[:, r:r + 1] == lanes, gatet[:, r:r + 1], 0.0)
            hi = w.astype(BF16)
            whi[:, r * 128:(r + 1) * 128] = hi
            wlo[:, r * 128:(r + 1) * 128] = (w - hi.astype(F32)).astype(BF16)

    def combine(k):
        rows = slice(CHUNKS[k][0], CHUNKS[k][0] + CHUNKS[k][1])
        if k:
            got(("back", k), G.at[rows])
        return dot(whi[:, rows], G[rows, :]) + dot(wlo[:, rows], G[rows, :])

    A, B = (0, 512), (512, 896)
    loads[1].wait()
    loads[2].wait()
    gate_up(0, *A)
    gate_up(0, *B)
    loads[3].wait()
    down_other(0)
    down_own(0)
    gather_x()
    weigh()
    forward(1)
    s0(0)
    forwarded(1)
    gate_up(1, *A)
    gather_z()
    gate_up(1, *B)
    down_other(1)
    down_own(1)
    s1(0)
    forward(2)
    forward(3)
    send_diagonal()
    s0(1)
    forwarded(2)
    gate_up(2, *A)
    gather_far()
    gate_up(2, *B)
    down_other(2)
    down_own(2)
    s1(1)
    s2(0)
    forwarded(3)
    gate_up(3, *A)
    s0(2)
    gate_up(3, *B)
    gather_end()
    down_other(3)
    send_last()
    down_own(3)
    gathered()
    gate_up(4, *A)
    s0(3)
    s1(2)
    gate_up(4, *B)
    down_other(4)
    s2(1)
    down_own(4)
    forward(6)
    forward(7)
    s0(4)
    forwarded(6)
    gate_up(5, *A)
    s1(3)
    gate_up(5, *B)
    down_other(5)
    s2(2)
    s3(0)
    down_own(5)
    forwarded(7)
    gate_up(6, *A)
    s0(5)
    s1(4)
    forward_last()
    gate_up(6, *B)
    down_other(6)
    s2(3)
    s3(1)
    down_own(6)
    forwarded_last()
    gate_up(7, *A)
    s0(6)
    gate_up(7, *B)
    s1(5)
    down_other(7)
    s2(4)
    s3(2)
    down_own(7)
    s0(7)
    s3(3)
    mixed[...] = combine(0) + combine(1) + combine(2)
    s1(6)
    s3(4)
    s3(5)
    s1(7)
    s3(6)
    s3(7)
    mixed[...] += combine(3) + combine(4) + combine(5)
    mixed[...] += combine(6)
    out_ref[...] = (mixed[...] + combine(7)).astype(BF16)
    assert len(slots) == N_RECV
    for cp in copies[-N_SEND:]:
        cp.wait_send()


N_SEND = 20
N_RECV = 66


def per_device(tokens, router_gates, routes, gate_proj, up_proj, down_proj):
    rows, width = tokens.shape
    hidden = gate_proj.shape[2]
    vmem = lambda *shape: pltpu.VMEM(shape, BF16)
    return pl.pallas_call(
        kernel,
        out_shape=jax.ShapeDtypeStruct((rows, 256), BF16),
        in_specs=[pl.BlockSpec(memory_space=pltpu.HBM)] * 6,
        out_specs=pl.BlockSpec(memory_space=pltpu.VMEM),
        scratch_shapes=[
            vmem(1024, width), vmem(width, hidden), vmem(width, hidden), vmem(hidden, width),
            vmem(rows, width), vmem(704, 2048), vmem(192, 256), vmem(256, hidden),
            vmem(2, 4, 2, 1024, 256), vmem(4, 2, 1024, 256),
            vmem(2, 1024, 256), vmem(3, 2, 1024, 256), vmem(1024, 256),
            vmem(4, 1024, 256), vmem(1024, 256), vmem(3, 1024, 256), vmem(1024, 256),
            vmem(1024, 256), vmem(256, 1024), vmem(256, 1024),
            pltpu.VMEM((2, 8, 256), F32), pltpu.VMEM((8, 256), F32), pltpu.VMEM((8, 256), F32),
            pltpu.VMEM((256, 256), F32), pltpu.VMEM((2, 256), jnp.int32), pltpu.VMEM((2, 256), F32),
            pltpu.SemaphoreType.DMA((N_SEND,)), pltpu.SemaphoreType.DMA((N_RECV,)),
            pltpu.SemaphoreType.DMA((6,)),
        ],
        compiler_params=pltpu.CompilerParams(
            collective_id=0, has_side_effects=True, vmem_limit_bytes=66 * 10**6
        ),
        name="layer",
    )(tokens, routes.T, router_gates.T, gate_proj[0], up_proj[0], down_proj[0])


def solution(mesh):
    in_specs = (
        P("expert", None),
        P("expert", None),
        P("expert", None),
        P("expert", None, "ffn"),
        P("expert", None, "ffn"),
        P("expert", "ffn", None),
    )
    out_specs = P("expert", "ffn")
    return jax.shard_map(
        per_device, mesh=mesh, in_specs=in_specs, out_specs=out_specs, check_vma=False
    )
```

```python
import jax
import jax.numpy as jnp
from jax import lax
from jax.experimental import pallas as pl
from jax.experimental.pallas import tpu as pltpu
from jax.sharding import PartitionSpec as P

MESH = pl.DeviceIdType.MESH
REL = ((0, 0), (0, 1), (1, 0), (3, 0), (2, 1), (2, 0), (1, 1), (3, 1))
CHUNKS = (
    (0, 128, 96, False), (128, 128, 128, False), (256, 128, 128, False), (384, 128, 128, False),
    (512, 128, 64, False), (768, 128, 48, True), (896, 128, 64, True), (640, 128, 64, True),
)
F32 = jnp.float32
BF16 = jnp.bfloat16


def dot(a, b):
    return jnp.dot(a, b, preferred_element_type=F32)


def kernel(
    tok_hbm, routes_hbm, gates_hbm, gate_hbm, up_hbm, down_hbm, out_ref,
    X, Wg, Wu, Wd, tok, OB, OP, hid, part, rD, rA1, rA2, rAx, rBx, rB1, rB2, G,
    placing, whi, wlo, keys, keyr, gater, mixed, routes, gates,
    send_sem, recv_sem, local_sem,
):
    e = lax.axis_index("expert")
    f = lax.axis_index("ffn")
    y, xl = e // 2, e % 2
    z, xh, c = f // 4, (f // 2) % 2, f % 2
    x = xh * 2 + xl

    def at(yy, xx, zz, cc):
        yy, xx, zz = yy % 4, xx % 4, zz % 4
        return {"expert": yy * 2 + xx % 2, "ffn": zz * 4 + (xx // 2) * 2 + cc}

    loads = [
        pltpu.make_async_copy(s, d, local_sem.at[i])
        for i, (s, d) in enumerate((
            (tok_hbm, tok), (gate_hbm, Wg), (up_hbm, Wu), (down_hbm, Wd), (routes_hbm, routes), (gates_hbm, gates),
        ))
    ]
    for i in (4, 5, 0):
        loads[i].start()

    barrier = pltpu.get_barrier_semaphore()
    peers = [
        at(y, x, z, 1 - c), at(y, x + 1, z, c), at(y, x + 3, z, c), at(y, x + 2, z, c),
        at(y + 1, x, z, c), at(y + 3, x, z, c), at(y + 2, x, z, c),
        at(y + 1, x + 1, z, c), at(y + 1, x + 3, z, c), at(y + 3, x + 1, z, c), at(y + 3, x + 3, z, c),
        at(y + 2, x + 1, z, c), at(y + 2, x + 3, z, c), at(y, x, z + 1, c), at(y, x, z + 3, c),
        at(y, x, z + 2, c),
    ]
    for dev in peers:
        pl.semaphore_signal(barrier, inc=1, device_id=dev, device_id_type=MESH)

    loads[4].wait()
    loads[5].wait()
    expert_ids = lax.broadcasted_iota(jnp.int32, (8, 256), 0)
    first, second = routes[0:1, :] == expert_ids, routes[1:2, :] == expert_ids
    chosen = jnp.where(first | second, 1.0, 0.0)
    earlier = lax.broadcasted_iota(jnp.int32, (256, 256), 0) < lax.broadcasted_iota(jnp.int32, (256, 256), 1)
    rank = dot(chosen.astype(BF16), jnp.where(earlier, 1.0, 0.0).astype(BF16))
    keys[0] = jnp.where(first | second, rank, -1.0)
    keys[1] = jnp.where(first, gates[0:1, :], 0.0) + jnp.where(second, gates[1:2, :], 0.0)
    row_ids = lax.broadcasted_iota(jnp.int32, (128, 256), 0).astype(F32)
    for r, (dy, dx) in enumerate(REL):
        owner = ((y + 4 - dy) % 4) * 2 + (xl + dx) % 2
        key = keys[0, pl.ds(owner, 1), :]
        keyr[r:r + 1, :] = key
        gater[r:r + 1, :] = keys[1, pl.ds(owner, 1), :]
        placing[r * 128:(r + 1) * 128, :] = jnp.where(key == row_ids, 1.0, 0.0).astype(BF16)

    copies = []
    slots = {}

    def send(src, dst, dev, key):
        i = len(copies)
        if i >= N_SEND:
            copies[i - N_SEND].wait_send()
        cp = pltpu.make_async_remote_copy(
            src_ref=src, dst_ref=dst, send_sem=send_sem.at[i % N_SEND],
            recv_sem=recv_sem.at[slots.setdefault(key, len(slots))], device_id=dev, device_id_type=MESH,
        )
        cp.start()
        copies.append(cp)

    def got(key, where):
        pltpu.make_async_copy(where, where, recv_sem.at[slots[key]]).wait()

    other = at(y, x, z, 1 - c)
    half = pl.multiple_of(c * 2048, 2048)

    def cols(b, width=256):
        return pl.ds(pl.multiple_of(b * 256, 256), width)

    x4 = (x + 1 + 2 * c) % 4
    block = c * 8 + z * 2 + xh
    block4 = c * 8 + z * 2 + x4 // 2
    loads[0].wait()
    loads[1].start()
    loads[2].start()
    OP[0:128, :] = dot(placing[512:640, :], tok[:, cols(block4)]).astype(BF16)
    OP[128:192, :] = dot(placing[640:704, :], tok[:, cols(block)]).astype(BF16)

    def place(lo, hi, to):
        def tile(t, carry):
            o = pl.multiple_of(t * 1024, 1024)
            v = dot(placing[lo:hi, :], tok[:, pl.ds(pl.multiple_of(half + o, 1024), 1024)])
            OB[to:to + hi - lo, pl.ds(o, 1024)] = v.astype(BF16)
            return carry

        lax.fori_loop(0, 2, tile, 0)

    def place_own(t, carry):
        o = pl.ds(pl.multiple_of(t * 1024, 1024), 1024)
        X[0:128, o] = dot(placing[0:128, :], tok[:, o]).astype(BF16)
        return carry

    outbox = {1: 0, 2: 128, 3: 256, 6: 448, 7: 576}
    place(128, 256, outbox[1])
    pl.semaphore_wait(barrier, len(peers))

    def quarter(r, yy, i):
        return send(
            OB.at[outbox[r]:outbox[r] + 128, i * 1024:(i + 1) * 1024],
            X.at[r * 128:(r + 1) * 128, pl.ds(pl.multiple_of(half + i * 1024, 1024), 1024)],
            at(yy, x + 1 + 2 * i, z, c), r,
        )

    def halves(r, yy):
        rows = slice(r * 128, (r + 1) * 128)
        send(OB.at[outbox[r]:outbox[r] + 128, :], X.at[rows, pl.ds(half, 2048)], at(yy, x, z, c), r)

    def send_diagonal():
        for r, yy, i in ((6, y + 3, 0), (7, y + 1, 1), (7, y + 1, 0), (6, y + 3, 1)):
            quarter(r, yy, i)

    send(OP.at[0:128], X.at[512:640, cols(block4)], at(y + 2, x4, z, c), 4)
    send(OP.at[128:192], X.at[640:704, cols(block)], at(y + 2, x, z, c), 5)
    quarter(1, y, 0)
    quarter(1, y, 1)
    place(256, 512, outbox[2])
    halves(2, y + 3)
    halves(3, y + 1)
    loads[3].start()
    place(704, 1024, 384)
    lax.fori_loop(0, 4, place_own, 0)

    def half_rows(lo, hi):
        return X.at[lo * 128:hi * 128, pl.ds(half, 2048)]

    def forward(r):
        got(r, half_rows(r, r + 1))
        send(half_rows(r, r + 1), half_rows(r, r + 1), other, ("core", r))

    def forwarded(r):
        got(("core", r), half_rows(r, r + 1))

    last = X.at[704:768, pl.ds(half, 2048)]

    def send_last():
        send(OB.at[384:448, :], last, at(y + 2, x, z, c), "last")

    def forward_last():
        got("last", last)
        send(last, last, other, ("core", 5))

    def forwarded_last():
        got(("core", 5), last)

    def spread(b, width, dev, key):
        where = X.at[512:704, cols(b, width)]
        send(where, where, dev, key)

    pair = lambda zz: c * 8 + (zz % 4) * 2
    xdev = at(y, x + 2, z, c)
    up_z, dn_z, far_z = at(y, x, z + 1, c), at(y, x, z + 3, c), at(y, x, z + 2, c)

    def gather_x():
        got(4, OP.at[0:128])
        got(5, OP.at[128:192])
        spread(block, 256, xdev, "x")

    def gather_z():
        got("x", X.at[512:704, 0:256])
        spread(pair(z), 512, up_z, "z")
        spread(pair(z), 512, dn_z, "z")
        spread(pair(z), 512, other, "c")

    def gather_far():
        got("z", X.at[512:704, 0:1024])
        spread(pair(z + 3), 256, up_z, "far")
        spread(pair(z + 1) + 1, 256, dn_z, "far")
        spread(pair(z + 1), 512, other, "c")
        spread(pair(z + 3), 512, other, "c")

    def gather_end():
        got("far", X.at[512:704, 0:512])
        spread(pair(z + 2), 512, other, "c")

    def gathered():
        got("c", X.at[512:704, pl.ds(half, 2048)])

    def gate_up(k, lo, hi):
        row, n = CHUNKS[k][:2]
        w = jnp.concatenate([Wg[:, lo:hi], Wu[:, lo:hi]], axis=1)
        both = dot(X[row:row + n, :], w)
        g, u = both[:, :hi - lo], both[:, hi - lo:]
        hid[0:n, lo:hi] = (g / (1.0 + jnp.exp(-g)) * u).astype(BF16)

    def down(k, cc):
        row, n = CHUNKS[k][:2]
        w = jnp.concatenate([Wd[:, cols(b * 2 + cc)] for b in range(8)], axis=1)
        v = dot(hid[0:n, :], w).astype(BF16)
        for b in range(8):
            part[cc, b // 2, b % 2, row:row + n, :] = v[:, b * 256:(b + 1) * 256]

    def down_other(k):
        rows = slice(CHUNKS[k][0], CHUNKS[k][0] + CHUNKS[k][1])
        down(k, 1 - c)
        send(part.at[1 - c, :, :, rows], rD.at[:, :, rows], other, ("d", k))

    def down_own(k):
        down(k, c)

    def add(dst, *srcs):
        total = dst[...].astype(F32)
        for s in srcs:
            total = total + s[...].astype(F32)
        dst[...] = total.astype(BF16)

    zp, zm, zf = (z + 1) % 4, (z + 3) % 4, (z + 2) % 4
    mine = part.at[c]

    def rows_of(k):
        row, n, a, _ = CHUNKS[k]
        mid = row + a
        return slice(row, mid), slice(mid, row + n), slice(mid, mid + (n - a) // 2), slice(mid + (n - a) // 2, row + n)

    def split(k):
        return CHUNKS[k][2] < CHUNKS[k][1]

    def direct(k):
        return CHUNKS[k][3]

    def s0(k):
        rows = slice(CHUNKS[k][0], CHUNKS[k][0] + CHUNKS[k][1])
        got(("d", k), rD.at[:, :, rows])
        a, b, _, _ = rows_of(k)

        def body(zz, carry):
            for xi in range(2):
                add(mine.at[zz, xi, rows], rD.at[zz, xi, rows])
            return carry

        lax.fori_loop(0, 4, body, 0)
        if split(k):
            send(mine.at[:, 1 - xh, b], rBx.at[:, b], xdev, ("bx", k))
        if direct(k):
            send(mine.at[zf, :, a], rA2.at[2, :, a], far_z, ("a2", k))
            send(mine.at[zp, :, a], rA2.at[0, :, a], up_z, ("a2", k))
            send(mine.at[zm, :, a], rA2.at[1, :, a], dn_z, ("a2", k))
        else:
            send(mine.at[zf, 0, a], rA1.at[0, a], up_z, ("a1", k))
            send(mine.at[zf, 1, a], rA1.at[1, a], dn_z, ("a1", k))

    def z_terms(k):
        return range(3 if direct(k) else 2)

    def x_first(k):
        _, b, lo, hi = rows_of(k)
        got(("bx", k), rBx.at[:, b])

        def body(zz, carry):
            add(mine.at[zz, xh, b], rBx.at[zz, b])
            return carry

        lax.fori_loop(0, 4, body, 0)
        if direct(k):
            send(mine.at[zf, xh, b], rB2.at[2, b], far_z, ("b2", k))
            send(mine.at[zp, xh, b], rB2.at[0, b], up_z, ("b2", k))
            send(mine.at[zm, xh, b], rB2.at[1, b], dn_z, ("b2", k))
        else:
            send(mine.at[zf, xh, lo], rB1.at[lo], up_z, ("b1", k))
            send(mine.at[zf, xh, hi], rB1.at[hi], dn_z, ("b1", k))

    def z_sum(k):
        a = rows_of(k)[0]
        got(("a2", k), rA2.at[0:len(z_terms(k)), :, a])
        add(mine.at[z, 1 - xh, a], *[rA2.at[i, 1 - xh, a] for i in z_terms(k)])
        send(mine.at[z, 1 - xh, a], rAx.at[a], xdev, ("ax", k))

    def s1(k):
        a = rows_of(k)[0]
        if direct(k):
            z_sum(k)
        else:
            got(("a1", k), rA1.at[:, a])
            add(mine.at[zp, 0, a], rA1.at[0, a])
            add(mine.at[zm, 1, a], rA1.at[1, a])
            send(mine.at[zp, :, a], rA2.at[0, :, a], up_z, ("a2", k))
            send(mine.at[zm, :, a], rA2.at[1, :, a], dn_z, ("a2", k))
        if split(k):
            x_first(k)

    def s2(k):
        _, b, lo, hi = rows_of(k)
        if split(k):
            got(("b1", k), rB1.at[b])
            add(mine.at[zp, xh, lo], rB1.at[lo])
            add(mine.at[zm, xh, hi], rB1.at[hi])
            send(mine.at[zp, xh, b], rB2.at[0, b], up_z, ("b2", k))
            send(mine.at[zm, xh, b], rB2.at[1, b], dn_z, ("b2", k))
        z_sum(k)

    def s3(k):
        row, n = CHUNKS[k][:2]
        a, b, _, _ = rows_of(k)
        if split(k):
            got(("b2", k), rB2.at[0:len(z_terms(k)), b])
            add(mine.at[z, xh, b], *[rB2.at[i, b] for i in z_terms(k)])
        got(("ax", k), rAx.at[a])
        add(mine.at[z, xh, a], rAx.at[a], *[rA2.at[i, xh, a] for i in z_terms(k)])
        for r in range(row // 128, (row + n) // 128):
            rows = slice(r * 128, (r + 1) * 128)
            dy, dx = REL[r]
            if r == 0:
                G[rows, :] = mine[z, xh, rows, :]
            else:
                owner = {"expert": ((y + dy) % 4) * 2 + (xl + dx) % 2, "ffn": f}
                send(mine.at[z, xh, rows], G.at[rows], owner, ("back", k))

    def weigh():
        keyt, gatet = keyr[...].T, gater[...].T
        lanes = lax.broadcasted_iota(jnp.int32, (256, 128), 1).astype(F32)
        for r in range(8):
            w = jnp.where(keyt[:, r:r + 1] == lanes, gatet[:, r:r + 1], 0.0)
            hi = w.astype(BF16)
            whi[:, r * 128:(r + 1) * 128] = hi
            wlo[:, r * 128:(r + 1) * 128] = (w - hi.astype(F32)).astype(BF16)

    def combine(k):
        rows = slice(CHUNKS[k][0], CHUNKS[k][0] + CHUNKS[k][1])
        if k:
            got(("back", k), G.at[rows])
        return dot(whi[:, rows], G[rows, :]) + dot(wlo[:, rows], G[rows, :])

    A, B = (0, 512), (512, 896)
    loads[1].wait()
    loads[2].wait()
    gate_up(0, *A)
    gate_up(0, *B)
    loads[3].wait()
    down_other(0)
    down_own(0)
    gather_x()
    weigh()
    forward(1)
    s0(0)
    forwarded(1)
    gate_up(1, *A)
    gather_z()
    gate_up(1, *B)
    down_other(1)
    down_own(1)
    s1(0)
    forward(2)
    forward(3)
    send_diagonal()
    s0(1)
    forwarded(2)
    gate_up(2, *A)
    gather_far()
    gate_up(2, *B)
    down_other(2)
    down_own(2)
    s1(1)
    s2(0)
    forwarded(3)
    gate_up(3, *A)
    s0(2)
    gate_up(3, *B)
    gather_end()
    down_other(3)
    send_last()
    down_own(3)
    gathered()
    gate_up(4, *A)
    s0(3)
    s1(2)
    gate_up(4, *B)
    down_other(4)
    s2(1)
    forward(6)
    down_own(4)
    forward(7)
    forwarded(6)
    gate_up(5, *A)
    s0(4)
    s1(3)
    gate_up(5, *B)
    down_other(5)
    s2(2)
    s3(0)
    down_own(5)
    forwarded(7)
    gate_up(6, *A)
    s0(5)
    s1(4)
    forward_last()
    gate_up(6, *B)
    down_other(6)
    s2(3)
    s3(1)
    down_own(6)
    forwarded_last()
    gate_up(7, *A)
    s0(6)
    gate_up(7, *B)
    s1(5)
    down_other(7)
    s2(4)
    s3(2)
    down_own(7)
    s0(7)
    s3(3)
    s1(6)
    s3(4)
    s3(5)
    s1(7)
    mixed[...] = combine(0) + combine(1) + combine(2)
    s3(6)
    s3(7)
    mixed[...] += combine(3) + combine(4) + combine(5)
    mixed[...] += combine(6)
    out_ref[...] = (mixed[...] + combine(7)).astype(BF16)
    assert len(slots) == N_RECV
    for cp in copies[-N_SEND:]:
        cp.wait_send()


N_SEND = 20
N_RECV = 66


def per_device(tokens, router_gates, routes, gate_proj, up_proj, down_proj):
    rows, width = tokens.shape
    hidden = gate_proj.shape[2]
    vmem = lambda *shape: pltpu.VMEM(shape, BF16)
    return pl.pallas_call(
        kernel,
        out_shape=jax.ShapeDtypeStruct((rows, 256), BF16),
        in_specs=[pl.BlockSpec(memory_space=pltpu.HBM)] * 6,
        out_specs=pl.BlockSpec(memory_space=pltpu.VMEM),
        scratch_shapes=[
            vmem(1024, width), vmem(width, hidden), vmem(width, hidden), vmem(hidden, width),
            vmem(rows, width), vmem(704, 2048), vmem(192, 256), vmem(256, hidden),
            vmem(2, 4, 2, 1024, 256), vmem(4, 2, 1024, 256),
            vmem(2, 1024, 256), vmem(3, 2, 1024, 256), vmem(1024, 256),
            vmem(4, 1024, 256), vmem(1024, 256), vmem(3, 1024, 256), vmem(1024, 256),
            vmem(1024, 256), vmem(256, 1024), vmem(256, 1024),
            pltpu.VMEM((2, 8, 256), F32), pltpu.VMEM((8, 256), F32), pltpu.VMEM((8, 256), F32),
            pltpu.VMEM((256, 256), F32), pltpu.VMEM((2, 256), jnp.int32), pltpu.VMEM((2, 256), F32),
            pltpu.SemaphoreType.DMA((N_SEND,)), pltpu.SemaphoreType.DMA((N_RECV,)),
            pltpu.SemaphoreType.DMA((6,)),
        ],
        compiler_params=pltpu.CompilerParams(
            collective_id=0, has_side_effects=True, vmem_limit_bytes=66 * 10**6
        ),
        name="layer",
    )(tokens, routes.T, router_gates.T, gate_proj[0], up_proj[0], down_proj[0])


def solution(mesh):
    in_specs = (
        P("expert", None),
        P("expert", None),
        P("expert", None),
        P("expert", None, "ffn"),
        P("expert", None, "ffn"),
        P("expert", "ffn", None),
    )
    out_specs = P("expert", "ffn")
    return jax.shard_map(
        per_device, mesh=mesh, in_specs=in_specs, out_specs=out_specs, check_vma=False
    )
```
